32 devices in a mesh: gx: 4 (over z), gy: 8 (over y, x, core).
Axes of the slice: x: 2, y: 2, z: 4, core: 2. Of those that a mesh axis runs over, the one named last changes fastest.
Arguments:
- tprime: float32 [256, 256, 128], P('gx', 'gy'), may hold values from -5 to 5
- vapor: float32 [256, 256, 128], P('gx', 'gy'), may hold values from -0.2 to 0.2
- wind_u: float32 [256, 256, 128], P('gx', 'gy'), may hold values from -2.5 to 2.5
- wind_v: float32 [256, 256, 128], P('gx', 'gy'), may hold values from -2.5 to 2.5
- wind_w: float32 [256, 256, 128], P('gx', 'gy'), may hold values from -2.5 to 2.5
- radius: float32 [32768, 128], P(('gx', 'gy')), may hold values from 4 to 20
- min_radius: float32 [32768, 128], P(('gx', 'gy')), may hold values from 1 to 4
- multiplicity: float32 [32768, 128], P(('gx', 'gy')), may hold values from 0.5 to 2
- drop_counts: int32 [32768], P(('gx', 'gy')), may hold values from 0 to 128, as said below
- cell_index: int32 [32768], P(('gx', 'gy')), may hold values from 0 to 262143
- move_list: int32 [32768], P(('gx', 'gy')), may hold values from -1 to 1023, as said below
Outputs:
- temperature_out: float32 [256, 256, 128], P('gx', 'gy')
- vapor_out: float32 [256, 256, 128], P('gx', 'gy')
- radius_out: float32 [16384, 128], P(('gx', 'gy'))
- multiplicity_out: float32 [16384, 128], P(('gx', 'gy'))
The draws below stay inside these ranges and needn't reach their ends.
Inputs may be any that keep to these rules, and one draw needn't show every extreme that they name: `move_list`: each entry is -1 for an empty home slot, else o * 32 + k: the block goes to owner o as the k-th block from its device to o. Within one device no value repeats, every owner receives exactly 512 blocks, some device holds 1024 live blocks and uses k = 31. `drop_counts`: 0 exactly in the home slots whose move_list entry is -1, else 1 to 128.
All inputs are finite; a program needn't handle non-finite values.
Results may differ from the reference program's by a relative error of at most 0.0003.
Values sent between devices are 32-bit elements; how exact they have to be, the bound alone decides.
No kernel may reach another device: no remote copies, remote signals or barrier semaphores. Data moves between devices by JAX's collectives and lax.ppermute only.
A program may use at most 64 MiB of HBM per device.

```python
import math
import jax
import jax.numpy as jnp
from jax import lax

CX = 64
CY = 32
CZ = 128
DROPS = 128
SUBSTEPS = 6
BLK_DEV = 512
HOME = 1024
CAP = 32
NX = 256
NY = 256
HOME_ALL = 32768
N_GX = 4
N_GY = 8
DEVICES = 32


def layout(key):
    base = jax.random.fold_in(key, 11)
    keys = jax.random.split(base, 5)
    half = DEVICES // 2
    shuffled = jax.random.permutation(keys[0], DEVICES).astype(jnp.int32)
    extra = jax.random.randint(keys[1], (half,), 0, HOME - BLK_DEV + 1, dtype=jnp.int32)
    extra = extra.at[0].set(HOME - BLK_DEV)
    loads = jnp.zeros((DEVICES,), jnp.int32).at[shuffled[0::2]].set(BLK_DEV + extra).at[shuffled[1::2]].set(BLK_DEV - extra)
    slot_keys = jax.random.split(keys[2], DEVICES)
    ranks = jax.vmap(lambda k: jax.random.permutation(k, HOME))(slot_keys).astype(jnp.int32)
    live = ranks < loads[:, None]
    within = (jnp.cumsum(live.astype(jnp.int32), axis=1) - 1).astype(jnp.int32)
    before = (jnp.cumsum(loads) - loads).astype(jnp.int32)
    global_rank = before[:, None] + within
    owners = jax.random.permutation(keys[3], DEVICES).astype(jnp.int32)
    owner = owners[global_rank % DEVICES]
    code = jnp.where(live, owner * CAP + within // DEVICES, -1).astype(jnp.int32)
    drawn = jax.random.randint(keys[4], (DEVICES, HOME), 1, DROPS + 1, dtype=jnp.int32)
    counts = jnp.where(live, drawn, 0).astype(jnp.int32)
    return (code.reshape(-1), counts.reshape(-1))


def draw_move_list(key, part):
    return layout(key)[0]


def draw_drop_counts(key, part):
    return layout(key)[1]


def with_ends(values, rng, smallest, largest):
    index_at = [jax.random.randint(jax.random.fold_in(rng, axis), (), 0, length) for axis, length in enumerate(values.shape)]
    main_axis = values.shape.index(max(values.shape))
    next_to = index_at[:main_axis] + [(index_at[main_axis] + 1) % values.shape[main_axis]] + index_at[main_axis + 1:]
    return values.at[tuple(index_at)].set(smallest).at[tuple(next_to)].set(largest)


def steps_of(stream_key, shape, cuts, smallest, high):
    factor_of = 1.0
    for axis_at, parts in cuts:
        draws = jax.random.uniform(jax.random.fold_in(jax.random.fold_in(stream_key, 6), axis_at), (parts,), jnp.float32, smallest / len(cuts), high / len(cuts))
        factor_of = factor_of * jnp.repeat(jnp.exp(draws), shape[axis_at] // parts).reshape((-1,) + (1,) * (len(shape) - 1 - axis_at))
    return factor_of


def gaussian(key, dims, deviation, bound, cuts=(), kind=jnp.bfloat16):
    values = deviation * jax.random.normal(key, dims, jnp.float32)
    if cuts:
        values = values * steps_of(key, dims, cuts, -0.22, 0.18)
    return jnp.clip(values, -bound, bound).astype(kind)


def setup_inputs(seed: int = 0) -> dict:
    seeds = jax.random.split(jax.random.key(seed), 12)
    tprime = gaussian(seeds[0], (NX, NY, CZ), 1.0, 5.0, ((0, 4), (1, 8)), jnp.float32)
    vapor = gaussian(seeds[1], (NX, NY, CZ), 0.03, 0.2, ((0, 4), (1, 8)), jnp.float32)
    wind_u = gaussian(seeds[2], (NX, NY, CZ), 0.4, 2.5, ((0, 4), (1, 8)), jnp.float32)
    wind_v = gaussian(seeds[3], (NX, NY, CZ), 0.4, 2.5, ((0, 4), (1, 8)), jnp.float32)
    wind_w = gaussian(seeds[4], (NX, NY, CZ), 0.4, 2.5, ((0, 4), (1, 8)), jnp.float32)
    radius = jnp.clip(jnp.exp(math.log(20.0) - 1.609438 * jax.random.uniform(seeds[5], (HOME_ALL, DROPS), jnp.float32) ** steps_of(seeds[5], (HOME_ALL, DROPS), ((0, 32),), -0.2, 0.2)), 4.0, 20.0)
    min_radius = jnp.clip(jnp.exp(math.log(4.0) - 1.3862944 * jax.random.uniform(seeds[6], (HOME_ALL, DROPS), jnp.float32) ** steps_of(seeds[6], (HOME_ALL, DROPS), ((0, 32),), -0.2, 0.2)), 1.0, 4.0)
    multiplicity = jnp.clip(jnp.exp(math.log(2.0) - 1.3862944 * jax.random.uniform(seeds[7], (HOME_ALL, DROPS), jnp.float32) ** steps_of(seeds[7], (HOME_ALL, DROPS), ((0, 32),), -0.2, 0.2)), 0.5, 2.0)
    drop_counts = draw_drop_counts(jax.random.fold_in(seeds[11], 71), 0)
    cell_index = with_ends(jax.random.randint(seeds[9], (HOME_ALL,), 0, CX * CY * CZ), jax.random.fold_in(seeds[9], 1), 0, (CX * CY * CZ) - 1).astype(jnp.int32)
    move_list = draw_move_list(jax.random.fold_in(seeds[11], 71), 0)
    return {"tprime": tprime, "vapor": vapor, "wind_u": wind_u, "wind_v": wind_v, "wind_w": wind_w, "radius": radius, "min_radius": min_radius, "multiplicity": multiplicity, "drop_counts": drop_counts, "cell_index": cell_index, "move_list": move_list}


clausius = 0.07
growth = 200.0 / 3.0
solute = 0.05
condense = 5e-07
latent = 10.0
collect = 1e-07
time_step = 2.0
advect_step = 0.6

def physics(radius, floor_radius, mult, cell_temp, cell_vapor):
    r2 = radius * radius
    floor2 = floor_radius * floor_radius
    temp = cell_temp
    wet = cell_vapor
    for _ in range(SUBSTEPS):
        sat = (1.0 + wet) * jnp.exp(-clausius * temp) - 1.0
        rad = jnp.sqrt(r2)
        ratio = floor_radius / rad
        grown = jnp.maximum(r2 + growth * (sat[:, None] + solute * ratio * ratio * ratio), floor2)
        condensed = lax.optimization_barrier(jnp.sum(mult * (grown * jnp.sqrt(grown) - r2 * rad), axis=1))
        wet = wet - condense * condensed
        temp = temp + latent * condense * condensed
        r2 = grown
    rad = jnp.sqrt(r2)
    mass = r2 * rad
    summed = rad[:, :, None] + rad[:, None, :]
    kernel = summed * summed * jnp.abs(r2[:, :, None] - r2[:, None, :])
    sweep = jnp.where(rad[:, :, None] > rad[:, None, :], kernel, 0.0)
    gain = collect * lax.optimization_barrier(jnp.sum(sweep * (mult * mass)[:, None, :], axis=2))
    loss = collect * lax.optimization_barrier(jnp.sum(sweep * mult[:, :, None], axis=1))
    radius_new = jnp.where(mult > 0.0, jnp.cbrt(mass + time_step * gain), 0.0)
    mult_new = mult * jnp.exp(-time_step * loss)
    heat = jnp.stack([temp - cell_temp, wet - cell_vapor], axis=1)
    return (radius_new, mult_new, heat)

def grouped(items, limit):
    count = items[0].shape[0]
    group = math.gcd(count, limit)

    def apply(pieces):
        return physics(*pieces)
    stacked = tuple((a.reshape((count // group, group) + a.shape[1:]) for a in items))
    result = lax.map(apply, stacked)
    return tuple((a.reshape((count,) + a.shape[2:]) for a in result))

def tendency(padded, along_x, along_y, along_z):
    middle_y = padded[:, :, 1:-1]
    flux_x = along_x * (0.5 * (middle_y[:, :-1] + middle_y[:, 1:]))
    middle_x = padded[:, 1:-1]
    flux_y = along_y * (0.5 * (middle_x[:, :, :-1] + middle_x[:, :, 1:]))
    core = padded[:, 1:-1, 1:-1]
    flux_z = along_z * (0.5 * (core[..., :-1] + core[..., 1:]))
    edge = jnp.zeros(core.shape[:-1] + (1,), core.dtype)
    flux_z = jnp.concatenate([edge, flux_z, edge], axis=-1)
    return -(flux_x[:, 1:] - flux_x[:, :-1]) - (flux_y[:, :, 1:] - flux_y[:, :, :-1]) - (flux_z[..., 1:] - flux_z[..., :-1])

def wrapped(stacked):
    return jnp.pad(stacked, ((0, 0), (1, 1), (1, 1), (0, 0)), mode='wrap')

def reference(tprime, vapor, wind_u, wind_v, wind_w, radius, min_radius, multiplicity, drop_counts, cell_index, move_list):
    devices = N_GX * N_GY
    home_all = radius.shape[0]
    blocks = jnp.arange(home_all, dtype=jnp.int32)
    device = (blocks // HOME).astype(jnp.int32)
    live = move_list >= 0
    owner = jnp.where(live, move_list // CAP, devices).astype(jnp.int32)
    column = (device * CAP + jnp.where(live, move_list % CAP, 0)).astype(jnp.int32)
    table = jnp.full((devices, devices * CAP), home_all, jnp.int32).at[owner, column].set(blocks, mode='drop')
    filled = table < home_all
    position = (jnp.cumsum(filled.astype(jnp.int32), axis=1) - 1).astype(jnp.int32)
    position = jnp.where(filled, position, BLK_DEV).astype(jnp.int32)
    rows = jnp.broadcast_to(jnp.arange(devices, dtype=jnp.int32)[:, None], table.shape)
    chosen = jnp.zeros((devices, BLK_DEV), jnp.int32).at[rows, position].set(table, mode='drop').reshape(-1)
    local_x = cell_index // (CY * CZ)
    local_y = cell_index // CZ % CY
    level = cell_index % CZ
    global_x = device // N_GY * CX + local_x
    global_y = device % N_GY * CY + local_y
    flat = ((global_x * NY + global_y) * CZ + level).astype(jnp.int32)
    cell_temp = tprime.reshape(-1)[flat]
    cell_vapor = vapor.reshape(-1)[flat]
    alive = jnp.arange(DROPS, dtype=jnp.int32)[None, :] < drop_counts[:, None]
    live_mult = jnp.where(alive, multiplicity, 0.0)
    radius_out, multiplicity_out, heat = grouped((radius[chosen], min_radius[chosen], live_mult[chosen], cell_temp[chosen], cell_vapor[chosen]), 256)
    home_heat = jnp.zeros((home_all, 2), heat.dtype).at[chosen].set(heat)
    heated_t = tprime.reshape(-1).at[flat].add(jnp.where(live, home_heat[:, 0], 0.0)).reshape(tprime.shape)
    heated_v = vapor.reshape(-1).at[flat].add(jnp.where(live, home_heat[:, 1], 0.0)).reshape(vapor.shape)
    winds = wrapped(jnp.stack([wind_u, wind_v]))
    along_x = 0.5 * (winds[0, :-1, 1:-1] + winds[0, 1:, 1:-1])
    along_y = 0.5 * (winds[1, 1:-1, :-1] + winds[1, 1:-1, 1:])
    along_z = 0.5 * (wind_w[..., :-1] + wind_w[..., 1:])
    start = jnp.stack([heated_t, heated_v])
    section = start
    for weight in (1.0 / 3.0, 0.5, 1.0):
        section = start + advect_step * weight * tendency(wrapped(section), along_x, along_y, along_z)
    return (section[0], section[1], radius_out, multiplicity_out)
```

```python
import jax
import jax.numpy as jnp
from jax import lax
from jax.experimental import pallas as pl
from jax.experimental.pallas import tpu as pltpu
from jax.sharding import PartitionSpec as P

SUBSTEPS = 6
BLK_DEV = 512
LAN = 128
SUB = 8
NV = 16
collect = 1e-07
time_step = 2.0
advect_step = 0.6
clausius = 0.07; growth = 200.0 / 3.0; solute = 0.05; condense = 5e-07; latent = 10.0
SMEM=lambda: pl.BlockSpec(memory_space=pltpu.SMEM)
VM=lambda: pl.BlockSpec(memory_space=pltpu.VMEM)

def row_loop(n, unroll, fn):
    def group(g,_):
        base=pl.multiple_of(g*unroll,unroll)
        for u in range(unroll):
            fn(base+u)
        return 0
    lax.fori_loop(0,n//unroll,group,0)

def place_kernel(move,count,mult,out,buf):
    n=mult.shape[0]
    buf[...]=jnp.zeros_like(buf)
    lane=lax.broadcasted_iota(jnp.int32,(1,LAN),1)
    def one(b):
        slot=move[b]
        dst=jnp.where(slot>=0,slot,n)
        buf[pl.ds(dst,1),:]=jnp.where(lane<count[b],mult[pl.ds(b,1),:],0.0)
    row_loop(n,8,one)
    out[...]=buf[:n,:]

def place(move,count,mult):
    n=mult.shape[0]
    return pl.pallas_call(place_kernel,out_shape=jax.ShapeDtypeStruct(mult.shape,jnp.float32),
        in_specs=[SMEM(),SMEM(),VM()],out_specs=VM(),
        scratch_shapes=[pltpu.VMEM((n+SUB,LAN),jnp.float32)],name="place")(move,count,mult)

def home_kernel(move,cell,count,level,radius,floor,mult,tp,vp,send,ht,hv,ct,cv,rows_t,rows_v,buf):
    n=radius.shape[0]
    def fetch(b):
        c=lax.shift_right_logical(cell[b],7)
        rows_t[pl.ds(b,1),:]=tp[pl.ds(c,1),:]
        rows_v[pl.ds(b,1),:]=vp[pl.ds(c,1),:]
    row_loop(n,8,fetch)
    depth=lax.broadcasted_iota(jnp.int32,(LAN,LAN),0)
    def tile(t,_):
        sl=pl.ds(pl.multiple_of(t*LAN,LAN),LAN)
        here=depth==level[pl.ds(t,1),:]
        temp0=jnp.sum(jnp.where(here,jnp.transpose(rows_t[sl,:]),0.0),axis=0,keepdims=True)
        wet0=jnp.sum(jnp.where(here,jnp.transpose(rows_v[sl,:]),0.0),axis=0,keepdims=True)
        r=jnp.transpose(radius[sl,:]); fl=jnp.transpose(floor[sl,:])
        m=jnp.where(depth<count[pl.ds(t,1),:],jnp.transpose(mult[sl,:]),0.0)
        r2=r*r; f2=fl*fl; g3=(growth*solute)*(f2*fl)
        inv=lax.rsqrt(r2); mass=r2*(r2*inv)
        temp=temp0; wet=wet0
        for k in range(SUBSTEPS):
            sat=(1.0+wet)*jnp.exp(-clausius*temp)-1.0
            grown=jnp.maximum(r2+(growth*sat+g3*(inv*inv*inv)),f2)
            inv=lax.rsqrt(grown)
            new=grown*(grown*inv)
            condensed=jnp.sum(m*(new-mass),axis=0,keepdims=True)
            wet=wet-condense*condensed
            temp=temp+latent*condense*condensed
            r2=grown; mass=new
        ht[pl.ds(t,1),:]=temp-temp0; hv[pl.ds(t,1),:]=wet-wet0
        ct[pl.ds(t,1),:]=temp0; cv[pl.ds(t,1),:]=wet0
        rows_t[sl,:]=jnp.transpose(r2)
        return 0
    lax.fori_loop(0,n//LAN,tile,0)
    buf[...]=jnp.zeros_like(buf)
    def put(b):
        slot=move[b]
        dst=jnp.where(slot>=0,slot,n)
        buf[pl.ds(dst,1),:]=rows_t[pl.ds(b,1),:]
    row_loop(n,8,put)
    send[...]=buf[:n,:]

def home(move,cell,count,radius,floor,mult,tp,vp):
    n=radius.shape[0]; g=n//LAN
    levels=tp.shape[-1]
    tab=jax.ShapeDtypeStruct((g,LAN),jnp.float32)
    return pl.pallas_call(home_kernel,
        out_shape=(jax.ShapeDtypeStruct(radius.shape,jnp.float32),tab,tab,tab,tab),
        in_specs=[SMEM(),SMEM()]+[VM()]*7,out_specs=(VM(),)*5,
        scratch_shapes=[pltpu.VMEM((n,LAN),jnp.float32),pltpu.VMEM((n,LAN),jnp.float32),pltpu.VMEM((n+SUB,LAN),jnp.float32)],
        name="home")(move,cell,count.reshape(g,LAN),(cell%levels).reshape(g,LAN),radius,floor,mult,
                     tp.reshape(-1,levels),vp.reshape(-1,levels))

def scatter_kernel(cell,cellv,ht,hv,ct,cv,tp,vp,ot,ov,vt,vv,acct,accv):
    g=cellv.shape[0]; n=g*LAN
    spread=lambda ref,t: jnp.transpose(jnp.broadcast_to(ref[pl.ds(t,1),:],(LAN,LAN)))
    acct[...]=jnp.zeros_like(acct); accv[...]=jnp.zeros_like(accv)
    def source(t,_):
        c=spread(cellv,t); a=spread(ht,t); b=spread(hv,t)
        for o in range(g):
            mine=cellv[o:o+1,:]
            st=jnp.zeros((SUB,LAN),jnp.float32); sv=st
            for k in range(LAN//SUB):
                same=c[k*SUB:(k+1)*SUB,:]==mine
                st=st+jnp.where(same,a[k*SUB:(k+1)*SUB,:],0.0)
                sv=sv+jnp.where(same,b[k*SUB:(k+1)*SUB,:],0.0)
            acct[o*SUB:(o+1)*SUB,:]+=st
            accv[o*SUB:(o+1)*SUB,:]+=sv
        return 0
    lax.fori_loop(0,g,source,0)
    def rows(t,_):
        sl=pl.ds(pl.multiple_of(t*LAN,LAN),LAN)
        s8=pl.ds(pl.multiple_of(t*SUB,SUB),SUB)
        nt=ct[pl.ds(t,1),:]+jnp.sum(acct[s8,:],axis=0,keepdims=True)
        nv=cv[pl.ds(t,1),:]+jnp.sum(accv[s8,:],axis=0,keepdims=True)
        vt[sl,:]=jnp.transpose(jnp.broadcast_to(nt,(LAN,LAN)))
        vv[sl,:]=jnp.transpose(jnp.broadcast_to(nv,(LAN,LAN)))
        return 0
    lax.fori_loop(0,g,rows,0)
    ot[...]=tp[...]; ov[...]=vp[...]
    lane=lax.broadcasted_iota(jnp.int32,(1,LAN),1)
    def put(b):
        x=cell[b]
        c=lax.shift_right_logical(x,7); hit=lane==(x&127)
        pltpu.store(ot.at[pl.ds(c,1),:],vt[pl.ds(b,1),:],mask=hit)
        pltpu.store(ov.at[pl.ds(c,1),:],vv[pl.ds(b,1),:],mask=hit)
    row_loop(n,8,put)

def scatter(cell,ht,hv,ct,cv,tp,vp):
    g=ht.shape[0]; n=g*LAN
    t2=tp.reshape(-1,LAN); v2=vp.reshape(-1,LAN)
    o=jax.ShapeDtypeStruct(t2.shape,jnp.float32)
    a,b=pl.pallas_call(scatter_kernel,out_shape=(o,o),in_specs=[SMEM()]+[VM()]*7,out_specs=(VM(),VM()),
        scratch_shapes=[pltpu.VMEM((n,LAN),jnp.float32)]*2+[pltpu.VMEM((g*SUB,LAN),jnp.float32)]*2,
        name="scatter")(cell,cell.reshape(g,LAN).astype(jnp.float32),ht,hv,ct,cv,t2,v2)
    return a.reshape(tp.shape),b.reshape(vp.shape)


def batcher(n):
    out=[]
    p=1
    while p<n:
        k=p
        while k>=1:
            for j in range(k%p, n-k, 2*k):
                for i in range(0, min(k, n-j-k)):
                    if (i+j)//(p*2)==(i+j+k)//(p*2):
                        out.append((i+j,i+j+k))
            k//=2
        p*=2
    return out
NET16=batcher(16)

def swap(keys, pays, a, b):
    c = keys[a] > keys[b]
    keys[a], keys[b] = jnp.where(c, keys[b], keys[a]), jnp.where(c, keys[a], keys[b])
    for p in pays:
        p[a], p[b] = jnp.where(c, p[b], p[a]), jnp.where(c, p[a], p[b])

def swap_min(keys, a, b):
    keys[a], keys[b] = jnp.minimum(keys[a], keys[b]), jnp.maximum(keys[a], keys[b])

def partner(x, j, upper):
    if j == 4:
        return pltpu.roll(x, 4, 0)
    return jnp.where(upper, pltpu.roll(x, j, 0), pltpu.roll(x, 8 - j, 0))

def sort128(keys, pays, row, flip):
    bit=[(row & 1) != 0, (row & 2) != 0, (row & 4) != 0]
    def flipped(mask):
        for v in range(NV):
            keys[v] = jnp.where(mask, flip(keys[v]), keys[v])
    flipped(bit[0])
    for a,b in NET16:
        swap(keys,pays,a,b) if pays else swap_min(keys,a,b)
    for lvl in range(3):
        nxt = bit[lvl+1] if lvl < 2 else None
        flipped(jnp.logical_xor(bit[lvl], nxt) if nxt is not None else bit[lvl])
        for s in range(lvl,-1,-1):
            j=1<<s; up=bit[s]
            for v in range(NV):
                pk=partner(keys[v],j,up)
                if pays:
                    c=jnp.logical_xor(keys[v]>pk, up)
                    keys[v]=jnp.where(c,pk,keys[v])
                    for p in pays:
                        p[v]=jnp.where(c,partner(p[v],j,up),p[v])
                else:
                    keys[v]=jnp.where(up, jnp.maximum(keys[v],pk), jnp.minimum(keys[v],pk))
        for d in (8,4,2,1):
            for a in range(NV):
                if a & d == 0:
                    swap(keys,pays,a,a|d) if pays else swap_min(keys,a,a|d)

def before(parts, row):
    run=None; excl=[]
    for x in parts:
        excl.append(run)
        run = x if run is None else run + x
    x=run
    for j in (1,2,4):
        x = x + jnp.where(row >= j, pltpu.roll(x, j, 0), 0.0)
    ahead = jnp.where(row >= 1, pltpu.roll(x, 1, 0), 0.0)
    total = jnp.sum(run, axis=0, keepdims=True)
    return [ahead if e is None else ahead + e for e in excl], total

def collect_tile(r2t, mt):
    row = lax.broadcasted_iota(jnp.int32,(SUB,LAN),0)
    keys=[]; m=[]
    for v in range(NV):
        q = row*16+v
        x = r2t[v*8:(v+1)*8,:]
        keys.append((x*16384.0).astype(jnp.int32)*128+q)
        m.append(mt[v*8:(v+1)*8,:])
    sort128(keys,[m],row,lambda k: -1-k)
    q=[k & 127 for k in keys]
    r2=[(lax.shift_right_logical(k,7)).astype(jnp.float32)*(1.0/16384.0) + (0.5/16384.0) for k in keys]
    rad=[jnp.sqrt(x) for x in r2]
    r3=[a*b for a,b in zip(r2,rad)]
    r4=[a*a for a in r2]
    m1=[a*b for a,b in zip(m,rad)]
    m3=[a*b for a,b in zip(m,r3)]
    m4=[a*b for a,b in zip(m,r4)]
    m6=[a*b for a,b in zip(m3,r3)]
    m7=[a*b for a,b in zip(m3,r4)]
    p0,t0=before(m,row); p1,t1=before(m1,row)
    p3,t3=before(m3,row); p4,t4=before(m4,row)
    p6,_=before(m6,row); p7,_=before(m7,row)
    outs_r=[]; outs_m=[]; key2=[]
    for v in range(NV):
        gain = collect*((r4[v]*p3[v]-p7[v]) + 2.0*(r3[v]*p4[v]-rad[v]*p6[v]))
        loss = collect*(((t4-p4[v]) - r4[v]*(t0-p0[v])) + 2.0*(rad[v]*(t3-p3[v]) - r3[v]*(t1-p1[v])))
        x = r3[v] + time_step*gain
        y = jnp.exp(jnp.log(x)*(1.0/3.0))
        y = y - (y*y*y - x)/(3.0*y*y)
        outs_r.append(jnp.where(m[v]>0.0, y, 0.0))
        outs_m.append(m[v]*jnp.exp(-time_step*loss))
        key2.append((q[v]*128 + (row + v*8)).astype(jnp.float32))
    sort128(key2,[],row,lambda k: -k)
    rank=[(key2[v]-(row*16+v).astype(jnp.float32)*128.0) for v in range(NV)]
    cat=lambda l: jnp.concatenate(l,axis=0)
    return cat(outs_r),cat(outs_m),cat(rank)


def receive_kernel(src, mults, r2s, ro_ref, mo_ref, mrow, rrow):
    blocks = ro_ref.shape[0]

    def pull(b):
        s = src[b]
        mrow[pl.ds(b, 1), :] = mults[pl.ds(s, 1), :]
        rrow[pl.ds(b, 1), :] = r2s[pl.ds(s, 1), :]

    row_loop(blocks, 8, pull)

    def tile(t, _):
        sl = pl.ds(pl.multiple_of(t * LAN, LAN), LAN)
        a, b, rank = collect_tile(jnp.transpose(rrow[sl, :]), jnp.transpose(mrow[sl, :]))
        rank = jnp.transpose(rank).astype(jnp.int32)
        ro_ref[sl, :] = jnp.take_along_axis(jnp.transpose(a), rank, axis=1)
        mo_ref[sl, :] = jnp.take_along_axis(jnp.transpose(b), rank, axis=1)
        return 0

    lax.fori_loop(0, blocks // LAN, tile, 0)


def receive(src, mults, r2s):
    out = jax.ShapeDtypeStruct((BLK_DEV, LAN), jnp.float32)
    return pl.pallas_call(
        receive_kernel,
        out_shape=(out, out),
        in_specs=[SMEM(), VM(), VM()],
        out_specs=(VM(), VM()),
        scratch_shapes=[pltpu.VMEM((BLK_DEV, LAN), jnp.float32)] * 2,
        name="receive",
    )(src, mults, r2s)


def sources(mults):
    taken = mults[:, 0] > 0.0
    position = jnp.cumsum(taken.astype(jnp.int32)) - 1
    hit = (position[None, :] == jnp.arange(BLK_DEV, dtype=jnp.int32)[:, None]) & taken[None, :]
    return jnp.sum(jnp.where(hit, jnp.arange(mults.shape[0], dtype=jnp.int32)[None, :], 0), axis=1)


def exchange(rows, devices):
    moved = lax.all_to_all(
        rows.reshape((devices, -1) + rows.shape[1:]), ("gx", "gy"), 0, 0, tiled=True
    )
    return moved.reshape(rows.shape)


def with_halo(array, sides, width):
    for axis, dim in sides:
        size, length = (lax.axis_size(axis), array.shape[dim])
        up = [(i, (i + 1) % size) for i in range(size)]
        down = [(j, i) for i, j in up]
        last = lax.slice_in_dim(array, length - width, length, axis=dim)
        first = lax.slice_in_dim(array, 0, width, axis=dim)
        before_ = lax.ppermute(last, axis, up)
        after_ = lax.ppermute(first, axis, down)
        array = jnp.concatenate([before_, array, after_], axis=dim)
    return array


def tendency(padded, along_x, along_y, along_z):
    middle_y = padded[:, :, 1:-1]
    flux_x = along_x * (0.5 * (middle_y[:, :-1] + middle_y[:, 1:]))
    middle_x = padded[:, 1:-1]
    flux_y = along_y * (0.5 * (middle_x[:, :, :-1] + middle_x[:, :, 1:]))
    core = padded[:, 1:-1, 1:-1]
    flux_z = along_z * (0.5 * (core[..., :-1] + core[..., 1:]))
    edge = jnp.zeros(core.shape[:-1] + (1,), core.dtype)
    flux_z = jnp.concatenate([edge, flux_z, edge], axis=-1)
    return (
        -(flux_x[:, 1:] - flux_x[:, :-1])
        - (flux_y[:, :, 1:] - flux_y[:, :, :-1])
        - (flux_z[..., 1:] - flux_z[..., :-1])
    )


def body(
    tprime,
    vapor,
    wind_u,
    wind_v,
    wind_w,
    radius,
    min_radius,
    multiplicity,
    drop_counts,
    cell_index,
    move_list,
):
    devices = lax.axis_size("gx") * lax.axis_size("gy")
    mults = exchange(place(move_list, drop_counts, multiplicity), devices)
    sent, ht, hv, ct, cv = home(
        move_list, cell_index, drop_counts, radius, min_radius, multiplicity, tprime, vapor
    )
    r2s = exchange(sent, devices)
    heated_t, heated_v = scatter(cell_index, ht, hv, ct, cv, tprime, vapor)
    radius_out, multiplicity_out = receive(sources(mults), mults, r2s)
    winds = with_halo(jnp.stack([wind_u, wind_v]), (("gx", 1), ("gy", 2)), 1)
    along_x = 0.5 * (winds[0, :-1, 1:-1] + winds[0, 1:, 1:-1])
    along_y = 0.5 * (winds[1, 1:-1, :-1] + winds[1, 1:-1, 1:])
    along_z = 0.5 * (wind_w[..., :-1] + wind_w[..., 1:])
    start = jnp.stack([heated_t, heated_v])
    section = start
    for weight in (1.0 / 3.0, 0.5, 1.0):
        section = start + advect_step * weight * tendency(
            with_halo(section, (("gx", 1), ("gy", 2)), 1), along_x, along_y, along_z
        )
    return (section[0], section[1], radius_out, multiplicity_out)


def solution(mesh):
    tile = P("gx", "gy", None)
    rows = P(("gx", "gy"), None)
    flat = P(("gx", "gy"))
    return jax.shard_map(
        body,
        mesh=mesh,
        in_specs=(tile,) * 5 + (rows,) * 3 + (flat,) * 3,
        out_specs=(tile, tile, rows, rows),
        check_vma=False,
    )
```

```python
import jax
import jax.numpy as jnp
from jax import lax
from jax.experimental import pallas as pl
from jax.experimental.pallas import tpu as pltpu
from jax.sharding import PartitionSpec as P

SUBSTEPS = 6
BLK_DEV = 512
LAN = 128
SUB = 8
NV = 16
collect = 1e-07
time_step = 2.0
advect_step = 0.6
clausius = 0.07; growth = 200.0 / 3.0; solute = 0.05; condense = 5e-07; latent = 10.0
SMEM=lambda: pl.BlockSpec(memory_space=pltpu.SMEM)
VM=lambda: pl.BlockSpec(memory_space=pltpu.VMEM)

def row_loop(n, unroll, fn):
    def group(g,_):
        base=pl.multiple_of(g*unroll,unroll)
        for u in range(unroll):
            fn(base+u)
        return 0
    lax.fori_loop(0,n//unroll,group,0)

def place_kernel(slot,mult,out,buf):
    n=mult.shape[0]
    buf[...]=jnp.zeros_like(buf)
    def one(b):
        buf[pl.ds(slot[b],1),:]=mult[pl.ds(b,1),:]
    row_loop(n,32,one)
    out[...]=buf[:n,:]

def place(slot,mult):
    n=mult.shape[0]
    return pl.pallas_call(place_kernel,out_shape=jax.ShapeDtypeStruct(mult.shape,jnp.float32),
        in_specs=[SMEM(),VM()],out_specs=VM(),
        scratch_shapes=[pltpu.VMEM((n+SUB,LAN),jnp.float32)],name="place")(slot,mult)

def home_kernel(slot,column,count,level,radius,floor,mult,tp,vp,send,ht,hv,ct,cv,rows_t,rows_v,buf):
    n=radius.shape[0]
    def fetch(b):
        c=column[b]
        rows_t[pl.ds(b,1),:]=tp[pl.ds(c,1),:]
        rows_v[pl.ds(b,1),:]=vp[pl.ds(c,1),:]
    row_loop(n,32,fetch)
    depth=lax.broadcasted_iota(jnp.int32,(LAN,LAN),0)
    def tile(t,_):
        sl=pl.ds(pl.multiple_of(t*LAN,LAN),LAN)
        here=depth==level[pl.ds(t,1),:]
        temp0=jnp.sum(jnp.where(here,jnp.transpose(rows_t[sl,:]),0.0),axis=0,keepdims=True)
        wet0=jnp.sum(jnp.where(here,jnp.transpose(rows_v[sl,:]),0.0),axis=0,keepdims=True)
        r=jnp.transpose(radius[sl,:]); fl=jnp.transpose(floor[sl,:])
        alive=depth<count[pl.ds(t,1),:]
        m=jnp.where(alive,jnp.transpose(mult[sl,:]),0.0)
        r2=r*r; f2=fl*fl; g3=(growth*solute)*(f2*fl)
        inv=lax.rsqrt(r2); mass=r2*(r2*inv)
        temp=temp0; wet=wet0
        for k in range(SUBSTEPS):
            sat=(1.0+wet)*jnp.exp(-clausius*temp)-1.0
            grown=jnp.maximum(r2+(growth*sat+g3*(inv*inv*inv)),f2)
            inv=lax.rsqrt(grown)
            new=grown*(grown*inv)
            condensed=jnp.sum(m*(new-mass),axis=0,keepdims=True)
            wet=wet-condense*condensed
            temp=temp+latent*condense*condensed
            r2=grown; mass=new
        ht[pl.ds(t,1),:]=temp-temp0; hv[pl.ds(t,1),:]=wet-wet0
        ct[pl.ds(t,1),:]=temp0; cv[pl.ds(t,1),:]=wet0
        rows_t[sl,:]=jnp.transpose(jnp.where(alive,r2,0.0))
        return 0
    lax.fori_loop(0,n//LAN,tile,0)
    buf[...]=jnp.zeros_like(buf)
    def put(b):
        buf[pl.ds(slot[b],1),:]=rows_t[pl.ds(b,1),:]
    row_loop(n,32,put)
    send[...]=buf[:n,:]

def home(slot,column,level,count,radius,floor,mult,tp,vp):
    n=radius.shape[0]; g=n//LAN
    levels=tp.shape[-1]
    tab=jax.ShapeDtypeStruct((g,LAN),jnp.float32)
    return pl.pallas_call(home_kernel,
        out_shape=(jax.ShapeDtypeStruct(radius.shape,jnp.float32),tab,tab,tab,tab),
        in_specs=[SMEM(),SMEM()]+[VM()]*7,out_specs=(VM(),)*5,
        scratch_shapes=[pltpu.VMEM((n,LAN),jnp.float32),pltpu.VMEM((n,LAN),jnp.float32),pltpu.VMEM((n+SUB,LAN),jnp.float32)],
        name="home")(slot,column,count.reshape(g,LAN),level.reshape(g,LAN),radius,floor,mult,
                     tp.reshape(-1,levels),vp.reshape(-1,levels))

def scatter_kernel(column,level,cellv,ht,hv,ct,cv,tp,vp,ot,ov,vt,vv,acct,accv):
    g=cellv.shape[0]; n=g*LAN
    spread=lambda ref,t: jnp.transpose(jnp.broadcast_to(ref[pl.ds(t,1),:],(LAN,LAN)))
    acct[...]=jnp.zeros_like(acct); accv[...]=jnp.zeros_like(accv)
    def source(t,_):
        c=spread(cellv,t); a=spread(ht,t); b=spread(hv,t)
        for o in range(g):
            mine=cellv[o:o+1,:]
            st=jnp.zeros((SUB,LAN),jnp.float32); sv=st
            for k in range(LAN//SUB):
                same=c[k*SUB:(k+1)*SUB,:]==mine
                st=st+jnp.where(same,a[k*SUB:(k+1)*SUB,:],0.0)
                sv=sv+jnp.where(same,b[k*SUB:(k+1)*SUB,:],0.0)
            acct[o*SUB:(o+1)*SUB,:]+=st
            accv[o*SUB:(o+1)*SUB,:]+=sv
        return 0
    lax.fori_loop(0,g,source,0)
    def rows(t,_):
        sl=pl.ds(pl.multiple_of(t*LAN,LAN),LAN)
        s8=pl.ds(pl.multiple_of(t*SUB,SUB),SUB)
        nt=ct[pl.ds(t,1),:]+jnp.sum(acct[s8,:],axis=0,keepdims=True)
        nv=cv[pl.ds(t,1),:]+jnp.sum(accv[s8,:],axis=0,keepdims=True)
        vt[sl,:]=jnp.transpose(jnp.broadcast_to(nt,(LAN,LAN)))
        vv[sl,:]=jnp.transpose(jnp.broadcast_to(nv,(LAN,LAN)))
        return 0
    lax.fori_loop(0,g,rows,0)
    ot[...]=tp[...]; ov[...]=vp[...]
    lane=lax.broadcasted_iota(jnp.int32,(1,LAN),1)
    def put(b):
        c=column[b]; hit=lane==level[b]
        pltpu.store(ot.at[pl.ds(c,1),:],vt[pl.ds(b,1),:],mask=hit)
        pltpu.store(ov.at[pl.ds(c,1),:],vv[pl.ds(b,1),:],mask=hit)
    row_loop(n,32,put)

def scatter(column,level,cell,ht,hv,ct,cv,tp,vp):
    g=ht.shape[0]; n=g*LAN
    t2=tp.reshape(-1,LAN); v2=vp.reshape(-1,LAN)
    o=jax.ShapeDtypeStruct(t2.shape,jnp.float32)
    a,b=pl.pallas_call(scatter_kernel,out_shape=(o,o),in_specs=[SMEM()]*2+[VM()]*7,out_specs=(VM(),VM()),
        scratch_shapes=[pltpu.VMEM((n,LAN),jnp.float32)]*2+[pltpu.VMEM((g*SUB,LAN),jnp.float32)]*2,
        name="scatter")(column,level,cell.reshape(g,LAN).astype(jnp.float32),ht,hv,ct,cv,t2,v2)
    return a.reshape(tp.shape),b.reshape(vp.shape)


def batcher(n):
    out=[]
    p=1
    while p<n:
        k=p
        while k>=1:
            for j in range(k%p, n-k, 2*k):
                for i in range(0, min(k, n-j-k)):
                    if (i+j)//(p*2)==(i+j+k)//(p*2):
                        out.append((i+j,i+j+k))
            k//=2
        p*=2
    return out
NET16=batcher(16)

def swap(keys, pays, a, b):
    c = keys[a] > keys[b]
    keys[a], keys[b] = jnp.where(c, keys[b], keys[a]), jnp.where(c, keys[a], keys[b])
    for p in pays:
        p[a], p[b] = jnp.where(c, p[b], p[a]), jnp.where(c, p[a], p[b])

def swap_min(keys, a, b):
    keys[a], keys[b] = jnp.minimum(keys[a], keys[b]), jnp.maximum(keys[a], keys[b])

def partner(x, j, upper):
    if j == 4:
        return pltpu.roll(x, 4, 0)
    return jnp.where(upper, pltpu.roll(x, j, 0), pltpu.roll(x, 8 - j, 0))

def sort128(keys, pays, row, flip):
    bit=[(row & 1) != 0, (row & 2) != 0, (row & 4) != 0]
    def flipped(mask):
        for v in range(NV):
            keys[v] = jnp.where(mask, flip(keys[v]), keys[v])
    flipped(bit[0])
    for a,b in NET16:
        swap(keys,pays,a,b) if pays else swap_min(keys,a,b)
    for lvl in range(3):
        nxt = bit[lvl+1] if lvl < 2 else None
        flipped(jnp.logical_xor(bit[lvl], nxt) if nxt is not None else bit[lvl])
        for s in range(lvl,-1,-1):
            j=1<<s; up=bit[s]
            for v in range(NV):
                pk=partner(keys[v],j,up)
                if pays:
                    c=jnp.logical_xor(keys[v]>pk, up)
                    keys[v]=jnp.where(c,pk,keys[v])
                    for p in pays:
                        p[v]=jnp.where(c,partner(p[v],j,up),p[v])
                else:
                    keys[v]=jnp.where(up, jnp.maximum(keys[v],pk), jnp.minimum(keys[v],pk))
        for d in (8,4,2,1):
            for a in range(NV):
                if a & d == 0:
                    swap(keys,pays,a,a|d) if pays else swap_min(keys,a,a|d)

def before(parts, row):
    run=None; excl=[]
    for x in parts:
        excl.append(run)
        run = x if run is None else run + x
    x=run
    for j in (1,2,4):
        x = x + jnp.where(row >= j, pltpu.roll(x, j, 0), 0.0)
    ahead = jnp.where(row >= 1, pltpu.roll(x, 1, 0), 0.0)
    total = jnp.sum(run, axis=0, keepdims=True)
    return [ahead if e is None else ahead + e for e in excl], total

def collect_tile(r2t, mt):
    row = lax.broadcasted_iota(jnp.int32,(SUB,LAN),0)
    keys=[]; m=[]
    for v in range(NV):
        q = row*16+v
        x = r2t[v*8:(v+1)*8,:]
        keys.append((x*16384.0).astype(jnp.int32)*128+q)
        m.append(mt[v*8:(v+1)*8,:])
    sort128(keys,[m],row,lambda k: -1-k)
    q=[k & 127 for k in keys]
    r2=[(lax.shift_right_logical(k,7)).astype(jnp.float32)*(1.0/16384.0) + (0.5/16384.0) for k in keys]
    rad=[jnp.sqrt(x) for x in r2]
    r3=[a*b for a,b in zip(r2,rad)]
    r4=[a*a for a in r2]
    m1=[a*b for a,b in zip(m,rad)]
    m3=[a*b for a,b in zip(m,r3)]
    m4=[a*b for a,b in zip(m,r4)]
    m6=[a*b for a,b in zip(m3,r3)]
    m7=[a*b for a,b in zip(m3,r4)]
    p0,t0=before(m,row); p1,t1=before(m1,row)
    p3,t3=before(m3,row); p4,t4=before(m4,row)
    p6,_=before(m6,row); p7,_=before(m7,row)
    outs_r=[]; outs_m=[]; key2=[]
    for v in range(NV):
        gain = collect*((r4[v]*p3[v]-p7[v]) + 2.0*(r3[v]*p4[v]-rad[v]*p6[v]))
        loss = collect*(((t4-p4[v]) - r4[v]*(t0-p0[v])) + 2.0*(rad[v]*(t3-p3[v]) - r3[v]*(t1-p1[v])))
        x = r3[v] + time_step*gain
        y = jnp.exp(jnp.log(x)*(1.0/3.0))
        y = y - (y*y*y - x)/(3.0*y*y)
        outs_r.append(jnp.where(m[v]>0.0, y, 0.0))
        outs_m.append(m[v]*jnp.exp(-time_step*loss))
        key2.append((q[v]*128 + (row + v*8)).astype(jnp.float32))
    sort128(key2,[],row,lambda k: -k)
    rank=[(key2[v]-(row*16+v).astype(jnp.float32)*128.0) for v in range(NV)]
    cat=lambda l: jnp.concatenate(l,axis=0)
    return cat(outs_r),cat(outs_m),cat(rank)


W=3
UNROLL=8

def advect_kernel(tc,vc,uc,vw,wc,xlo,xhi,ylo,yhi,ot,ov,f,ax,ay,az,ad,s1,s2,sem):
    nx,ny,_=tc.shape
    nt=ny//SUB+1
    copies=[pltpu.make_async_copy(c,f.at[i,pl.ds(W,nx),pl.ds(0,ny)],sem.at[i]) for i,c in enumerate((tc,vc,uc,vw,wc))]
    for c in copies: c.start()
    def sides(x,_):
        for i in range(5):
            f[i,x,ny:ny+W,:]=yhi[i,x]
            f[i,x,ny+SUB-W:ny+SUB,:]=ylo[i,x]
        return 0
    lax.fori_loop(0,nx+2*W,sides,0)
    for i in range(5):
        f[i,0:W,0:ny,:]=xlo[i]
        f[i,W+nx:W+nx+W,0:ny,:]=xhi[i]
    for c in copies: c.wait()
    scale=0.25*advect_step
    lane=lax.broadcasted_iota(jnp.int32,(SUB,LAN),1)
    first=lane==0; last=lane==LAN-1
    row=lax.broadcasted_iota(jnp.int32,(SUB,LAN),0)
    bottom=row==SUB-1; top=row==0
    rows=lambda t: pl.ds(t*SUB,SUB)
    near=pair_matrix()
    def ahead(tl):
        r=[pltpu.roll(x,SUB-1,0) for x in tl]
        return [jnp.where(bottom,r[(t+1)%nt],r[t]) for t in range(nt)]
    def behind(tl):
        r=[pltpu.roll(x,1,0) for x in tl]
        return [jnp.where(top,r[t-1],r[t]) for t in range(nt)]
    def pairs(tl):
        x=jnp.concatenate(tl,axis=0)
        hi=x.astype(jnp.bfloat16)
        lo=(x-hi.astype(jnp.float32)).astype(jnp.bfloat16)
        y=jnp.dot(jnp.concatenate([hi,lo],axis=1),near,preferred_element_type=jnp.float32)
        return [(y[k*SUB:(k+1)*SUB,:LAN],y[k*SUB:(k+1)*SUB,LAN:]) for k in range(len(tl))]
    def coef(g,_):
        x0=g*UNROLL
        zs=pairs([f[4,x0+p,rows(t),:] for p in range(UNROLL) for t in range(nt)])
        for p in range(UNROLL):
            x=x0+p
            xn=x+1
            for t in range(nt):
                ax[x,rows(t),:]=scale*(f[2,x,rows(t),:]+f[2,xn,rows(t),:])
            v=[f[3,x,rows(t),:] for t in range(nt)]
            for t,n in enumerate(ahead(v)):
                ay[x,rows(t),:]=scale*(v[t]+n)
            for t in range(nt):
                up,dn=zs[p*nt+t]
                az[x,rows(t),:]=jnp.where(last,0.0,scale*up)
                ad[x,rows(t),:]=jnp.where(first,0.0,scale*dn)
        return 0
    lax.fori_loop(0,pl.cdiv(nx+2*W,UNROLL),coef,0)
    def section(weight,src,dst,margin,count):
        edge=tuple(ax[margin-1,rows(t),:]*(src[i,margin-1,rows(t),:]+src[i,margin,rows(t),:]) for i in range(2) for t in range(count))
        def planes(g,prev):
            x0=margin+g*UNROLL
            f0={(i,p):[src[i,x0+p,rows(t),:] for t in range(nt)] for i in range(2) for p in range(UNROLL+1)}
            zs=[pairs([f0[i,p][t] for p in range(UNROLL) for t in range(count)]) for i in range(2)]
            for p in range(UNROLL):
                x=x0+p; nxt=[]
                for i in range(2):
                    c=f0[i,p]; up=ahead(c)
                    gy=[ay[x,rows(t),:]*(c[t]+up[t]) for t in range(nt)]
                    dn=behind(gy)
                    for t in range(count):
                        gx=ax[x,rows(t),:]*(c[t]+f0[i,p+1][t])
                        zu,zd=zs[i][p*count+t]
                        d=(gx-prev[i*count+t])+(gy[t]-dn[t])+(az[x,rows(t),:]*zu-ad[x,rows(t),:]*zd)
                        dst(i,x,t,f[i,x,rows(t),:]-weight*d)
                        nxt.append(gx)
                prev=tuple(nxt)
            return prev
        lax.fori_loop(0,pl.cdiv(nx+2*W-2*margin,UNROLL),planes,edge)
    def put(buf):
        def g(i,x,t,val): buf[i,x,rows(t),:]=val
        return g
    def out(i,x,t,val):
        (ot,ov)[i][x-W,rows(t),:]=val
    section(1.0/3.0,f,put(s1),1,nt)
    section(0.5,s1,put(s2),2,nt)
    section(1.0,s2,out,3,nt-1)

def pair_matrix():
    k=lax.broadcasted_iota(jnp.int32,(2*LAN,2*LAN),0)
    n=lax.broadcasted_iota(jnp.int32,(2*LAN,2*LAN),1)
    z=jnp.where(k>=LAN,k-LAN,k)
    o=jnp.where(n>=LAN,n-LAN,n)
    other=jnp.where(n>=LAN,o-1,o+1)
    return jnp.where((z==o)|(z==other),1.0,0.0).astype(jnp.bfloat16)

def advect(t,v,u,w2,w3,xlo,xhi,ylo,yhi):
    nx,ny,nz=t.shape
    o=jax.ShapeDtypeStruct(t.shape,jnp.float32)
    ext=(pl.cdiv(nx+2*W,UNROLL)*UNROLL+SUB,ny+SUB,nz)
    ANY=pl.BlockSpec(memory_space=pl.ANY); VM=pl.BlockSpec(memory_space=pltpu.VMEM)
    return pl.pallas_call(advect_kernel,out_shape=(o,o),in_specs=[ANY]*5+[VM]*4,out_specs=(VM,VM),
        scratch_shapes=[pltpu.VMEM((5,)+ext,jnp.float32)]+[pltpu.VMEM(ext,jnp.float32)]*4+[pltpu.VMEM((2,)+ext,jnp.float32)]*2+[pltpu.SemaphoreType.DMA((5,))],
        name="advect")(t,v,u,w2,w3,xlo,xhi,ylo,yhi)


def receive_kernel(src, mults, r2s, ro_ref, mo_ref, mrow, rrow):
    blocks = ro_ref.shape[0]

    def pull(b):
        s = src[b]
        mrow[pl.ds(b, 1), :] = mults[pl.ds(s, 1), :]
        rrow[pl.ds(b, 1), :] = r2s[pl.ds(s, 1), :]

    row_loop(blocks, 32, pull)

    def tile(t, _):
        sl = pl.ds(pl.multiple_of(t * LAN, LAN), LAN)
        r2 = jnp.transpose(rrow[sl, :])
        a, b, rank = collect_tile(r2, jnp.where(r2 > 0.0, jnp.transpose(mrow[sl, :]), 0.0))
        rank = jnp.transpose(rank).astype(jnp.int32)
        ro_ref[sl, :] = jnp.take_along_axis(jnp.transpose(a), rank, axis=1)
        mo_ref[sl, :] = jnp.take_along_axis(jnp.transpose(b), rank, axis=1)
        return 0

    lax.fori_loop(0, blocks // LAN, tile, 0)


def receive(src, mults, r2s):
    out = jax.ShapeDtypeStruct((BLK_DEV, LAN), jnp.float32)
    return pl.pallas_call(
        receive_kernel,
        out_shape=(out, out),
        in_specs=[SMEM(), VM(), VM()],
        out_specs=(VM(), VM()),
        scratch_shapes=[pltpu.VMEM((BLK_DEV, LAN), jnp.float32)] * 2,
        name="receive",
    )(src, mults, r2s)


def sources(mults):
    taken = mults[:, 0] > 0.0
    position = jnp.cumsum(taken.astype(jnp.int32)) - 1
    hit = (position[None, :] == jnp.arange(BLK_DEV, dtype=jnp.int32)[:, None]) & taken[None, :]
    return jnp.sum(jnp.where(hit, jnp.arange(mults.shape[0], dtype=jnp.int32)[None, :], 0), axis=1)


def exchange(rows, devices):
    moved = lax.all_to_all(
        rows.reshape((devices, -1) + rows.shape[1:]), ("gx", "gy"), 0, 0, tiled=True
    )
    return moved.reshape(rows.shape)


def shifts(axis):
    size = lax.axis_size(axis)
    up = [(i, (i + 1) % size) for i in range(size)]
    return up, [(j, i) for i, j in up]


def slabs(arrays, dim, start):
    return jnp.stack([lax.slice_in_dim(a, start, start + W, axis=dim) for a in arrays])


def halos(arrays):
    nx, ny = arrays[0].shape[:2]
    up, down = shifts("gx")
    xlo = lax.ppermute(slabs(arrays, 0, nx - W), "gx", up)
    xhi = lax.ppermute(slabs(arrays, 0, 0), "gx", down)
    up, down = shifts("gy")

    def side(start):
        ends = [x[:, :, start : start + W] for x in (xlo, xhi)]
        return jnp.concatenate([ends[0], slabs(arrays, 1, start), ends[1]], axis=1)

    ylo = lax.ppermute(side(ny - W), "gy", up)
    yhi = lax.ppermute(side(0), "gy", down)
    return xlo, xhi, ylo, yhi


def body(
    tprime,
    vapor,
    wind_u,
    wind_v,
    wind_w,
    radius,
    min_radius,
    multiplicity,
    drop_counts,
    cell_index,
    move_list,
):
    devices = lax.axis_size("gx") * lax.axis_size("gy")
    levels = tprime.shape[2]
    slot = jnp.where(move_list >= 0, move_list, multiplicity.shape[0])
    column = cell_index // levels
    level = cell_index % levels
    mults = exchange(place(slot, multiplicity), devices)
    sent, ht, hv, ct, cv = home(
        slot, column, level, drop_counts, radius, min_radius, multiplicity, tprime, vapor
    )
    r2s = exchange(sent, devices)
    heated_t, heated_v = scatter(column, level, cell_index, ht, hv, ct, cv, tprime, vapor)
    fields = (heated_t, heated_v, wind_u, wind_v, wind_w)
    temperature_out, vapor_out = advect(*fields, *halos(fields))
    radius_out, multiplicity_out = receive(sources(mults), mults, r2s)
    return (temperature_out, vapor_out, radius_out, multiplicity_out)


def solution(mesh):
    tile = P("gx", "gy", None)
    rows = P(("gx", "gy"), None)
    flat = P(("gx", "gy"))
    return jax.shard_map(
        body,
        mesh=mesh,
        in_specs=(tile,) * 5 + (rows,) * 3 + (flat,) * 3,
        out_specs=(tile, tile, rows, rows),
        check_vma=False,
    )
```

```python
import jax
import jax.numpy as jnp
from jax import lax
from jax.experimental import pallas as pl
from jax.experimental.pallas import tpu as pltpu
from jax.sharding import PartitionSpec as P

SUBSTEPS = 6
BLK_DEV = 512
LAN = 128
SUB = 8
NV = 16
collect = 1e-07
time_step = 2.0
advect_step = 0.6
clausius = 0.07; growth = 200.0 / 3.0; solute = 0.05; condense = 5e-07; latent = 10.0
SMEM=lambda: pl.BlockSpec(memory_space=pltpu.SMEM)
ANY=lambda: pl.BlockSpec(memory_space=pl.ANY)
VM=lambda: pl.BlockSpec(memory_space=pltpu.VMEM)

def row_loop(n, unroll, fn):
    def group(g,_):
        base=pl.multiple_of(g*unroll,unroll)
        for u in range(unroll):
            fn(base+u)
        return 0
    lax.fori_loop(0,n//unroll,group,0)

def place_kernel(slot,mult,out,buf):
    n=mult.shape[0]
    buf[...]=jnp.zeros_like(buf)
    def one(b):
        buf[pl.ds(slot[b],1),:]=mult[pl.ds(b,1),:]
    row_loop(n,32,one)
    out[...]=buf[:n,:]

def place(slot,mult):
    n=mult.shape[0]
    return pl.pallas_call(place_kernel,out_shape=jax.ShapeDtypeStruct(mult.shape,jnp.float32),
        in_specs=[SMEM(),VM()],out_specs=VM(),
        scratch_shapes=[pltpu.VMEM((n+SUB,LAN),jnp.float32)],name="place")(slot,mult)

def home_kernel(slot,column,count,level,radius_,floor_,mult_,tp_,vp_,send,ht,hv,ct,cv,rows_t,rows_v,buf,radius,floor,mult,tp,vp,sem):
    n=radius.shape[0]
    pairs_=((tp_,tp),(vp_,vp),(radius_,radius),(floor_,floor),(mult_,mult))
    loads=[pltpu.make_async_copy(a,b,sem.at[i]) for i,(a,b) in enumerate(pairs_)]
    for c in loads: c.start()
    buf[...]=jnp.zeros_like(buf)
    for c in loads[:2]: c.wait()
    def fetch(b):
        c=column[b]
        rows_t[pl.ds(b,1),:]=tp[pl.ds(c,1),:]
        rows_v[pl.ds(b,1),:]=vp[pl.ds(c,1),:]
    row_loop(n,32,fetch)
    for c in loads[2:]: c.wait()
    depth=lax.broadcasted_iota(jnp.int32,(LAN,LAN),0)
    def tile(t,_):
        sl=pl.ds(pl.multiple_of(t*LAN,LAN),LAN)
        here=depth==level[pl.ds(t,1),:]
        temp0=jnp.sum(jnp.where(here,jnp.transpose(rows_t[sl,:]),0.0),axis=0,keepdims=True)
        wet0=jnp.sum(jnp.where(here,jnp.transpose(rows_v[sl,:]),0.0),axis=0,keepdims=True)
        r=jnp.transpose(radius[sl,:]); fl=jnp.transpose(floor[sl,:])
        alive=depth<count[pl.ds(t,1),:]
        m=jnp.where(alive,jnp.transpose(mult[sl,:]),0.0)
        r2=r*r; f2=fl*fl; g3=(growth*solute)*(f2*fl)
        inv=lax.rsqrt(r2); mass=r2*(r2*inv)
        temp=temp0; wet=wet0
        for k in range(SUBSTEPS):
            sat=(1.0+wet)*jnp.exp(-clausius*temp)-1.0
            grown=jnp.maximum(r2+(growth*sat+g3*(inv*inv*inv)),f2)
            inv=lax.rsqrt(grown)
            new=grown*(grown*inv)
            condensed=jnp.sum(m*(new-mass),axis=0,keepdims=True)
            wet=wet-condense*condensed
            temp=temp+latent*condense*condensed
            r2=grown; mass=new
        ht[pl.ds(t,1),:]=temp-temp0; hv[pl.ds(t,1),:]=wet-wet0
        ct[pl.ds(t,1),:]=temp0; cv[pl.ds(t,1),:]=wet0
        rows_t[sl,:]=jnp.transpose(jnp.where(alive,r2,0.0))
        return 0
    lax.fori_loop(0,n//LAN,tile,0)
    def put(b):
        buf[pl.ds(slot[b],1),:]=rows_t[pl.ds(b,1),:]
    row_loop(n,32,put)
    send[...]=buf[:n,:]

def home(slot,column,level,count,radius,floor,mult,tp,vp):
    n=radius.shape[0]; g=n//LAN
    levels=tp.shape[-1]
    tab=jax.ShapeDtypeStruct((g,LAN),jnp.float32)
    return pl.pallas_call(home_kernel,
        out_shape=(jax.ShapeDtypeStruct(radius.shape,jnp.float32),tab,tab,tab,tab),
        in_specs=[SMEM(),SMEM(),VM(),VM()]+[ANY()]*5,out_specs=(VM(),)*5,
        scratch_shapes=[pltpu.VMEM((n,LAN),jnp.float32)]*2+[pltpu.VMEM((n+SUB,LAN),jnp.float32)]+[pltpu.VMEM((n,LAN),jnp.float32)]*3+[pltpu.VMEM((tp.size//levels,levels),jnp.float32)]*2+[pltpu.SemaphoreType.DMA((5,))],
        name="home")(slot,column,count.reshape(g,LAN),level.reshape(g,LAN),radius,floor,mult,
                     tp.reshape(-1,levels),vp.reshape(-1,levels))

def scatter_kernel(column,level,cellv,ht,hv,ct,cv,tp,vp,wu,wv,ww,ot,ov,xfirst,xlast,yfirst,ylast,vt,vv,acct,accv,wlo,whi,sem):
    g=cellv.shape[0]; n=g*LAN
    nx,ny=tp.shape[:2]
    winds=(wu,wv,ww)
    loads=[pltpu.make_async_copy(tp,ot,sem.at[0]),pltpu.make_async_copy(vp,ov,sem.at[1])]
    for i,w in enumerate(winds):
        loads+=[pltpu.make_async_copy(w.at[:,pl.ds(0,SUB)],wlo.at[i],sem.at[2+i]),
                pltpu.make_async_copy(w.at[:,pl.ds(ny-SUB,SUB)],whi.at[i],sem.at[5+i]),
                pltpu.make_async_copy(w.at[pl.ds(0,W)],xfirst.at[2+i],sem.at[8+i]),
                pltpu.make_async_copy(w.at[pl.ds(nx-W,W)],xlast.at[2+i],sem.at[11+i])]
    for c in loads: c.start()
    spread=lambda ref,t: jnp.transpose(jnp.broadcast_to(ref[pl.ds(t,1),:],(LAN,LAN)))
    acct[...]=jnp.zeros_like(acct); accv[...]=jnp.zeros_like(accv)
    def source(t,_):
        c=spread(cellv,t); a=spread(ht,t); b=spread(hv,t)
        for o in range(g):
            mine=cellv[o:o+1,:]
            st=jnp.zeros((SUB,LAN),jnp.float32); sv=st
            for k in range(LAN//SUB):
                same=c[k*SUB:(k+1)*SUB,:]==mine
                st=st+jnp.where(same,a[k*SUB:(k+1)*SUB,:],0.0)
                sv=sv+jnp.where(same,b[k*SUB:(k+1)*SUB,:],0.0)
            acct[o*SUB:(o+1)*SUB,:]+=st
            accv[o*SUB:(o+1)*SUB,:]+=sv
        return 0
    lax.fori_loop(0,g,source,0)
    def rows(t,_):
        sl=pl.ds(pl.multiple_of(t*LAN,LAN),LAN)
        s8=pl.ds(pl.multiple_of(t*SUB,SUB),SUB)
        nt=ct[pl.ds(t,1),:]+jnp.sum(acct[s8,:],axis=0,keepdims=True)
        nv=cv[pl.ds(t,1),:]+jnp.sum(accv[s8,:],axis=0,keepdims=True)
        vt[sl,:]=jnp.transpose(jnp.broadcast_to(nt,(LAN,LAN)))
        vv[sl,:]=jnp.transpose(jnp.broadcast_to(nv,(LAN,LAN)))
        return 0
    lax.fori_loop(0,g,rows,0)
    for c in loads: c.wait()
    lane=lax.broadcasted_iota(jnp.int32,(1,LAN),1)
    flat_t=ot.reshape(nx*ny,LAN); flat_v=ov.reshape(nx*ny,LAN)
    def put(b):
        c=column[b]; hit=lane==level[b]
        pltpu.store(flat_t.at[pl.ds(c,1),:],vt[pl.ds(b,1),:],mask=hit)
        pltpu.store(flat_v.at[pl.ds(c,1),:],vv[pl.ds(b,1),:],mask=hit)
    row_loop(n,32,put)
    for i,o in enumerate((ot,ov)):
        xfirst[i]=o[0:W]; xlast[i]=o[nx-W:nx]
    def side(x,_):
        at=pl.ds(x*W,W)
        for i,o in enumerate((ot,ov)):
            yfirst[i,at,:]=o[x,0:W,:]; ylast[i,at,:]=o[x,ny-W:ny,:]
        for i in range(3):
            yfirst[2+i,at,:]=wlo[i,x,0:W,:]; ylast[2+i,at,:]=whi[i,x,SUB-W:SUB,:]
        return 0
    lax.fori_loop(0,nx,side,0,unroll=4)

def scatter(column,level,cell,ht,hv,ct,cv,tp,vp,*winds):
    g=ht.shape[0]; n=g*LAN
    nx,ny,nz=tp.shape
    S=lambda *d: jax.ShapeDtypeStruct(d,jnp.float32)
    return pl.pallas_call(scatter_kernel,out_shape=(S(nx,ny,nz),)*2+(S(5,W,ny,nz),)*2+(S(5,nx*W,nz),)*2,
        in_specs=[SMEM()]*2+[VM()]*5+[ANY()]*5,out_specs=(VM(),)*6,
        scratch_shapes=[pltpu.VMEM((n,LAN),jnp.float32)]*2+[pltpu.VMEM((g*SUB,LAN),jnp.float32)]*2
            +[pltpu.VMEM((3,nx,SUB,nz),jnp.float32)]*2+[pltpu.SemaphoreType.DMA((14,))],
        name="scatter")(column,level,cell.reshape(g,LAN).astype(jnp.float32),ht,hv,ct,cv,tp,vp,*winds)


def batcher(n):
    out=[]
    p=1
    while p<n:
        k=p
        while k>=1:
            for j in range(k%p, n-k, 2*k):
                for i in range(0, min(k, n-j-k)):
                    if (i+j)//(p*2)==(i+j+k)//(p*2):
                        out.append((i+j,i+j+k))
            k//=2
        p*=2
    return out
NET16=batcher(16)

def swap(keys, pays, a, b):
    c = keys[a] > keys[b]
    keys[a], keys[b] = jnp.where(c, keys[b], keys[a]), jnp.where(c, keys[a], keys[b])
    for p in pays:
        p[a], p[b] = jnp.where(c, p[b], p[a]), jnp.where(c, p[a], p[b])

def swap_min(keys, a, b):
    keys[a], keys[b] = jnp.minimum(keys[a], keys[b]), jnp.maximum(keys[a], keys[b])

def partner(x, j, upper):
    if j == 4:
        return pltpu.roll(x, 4, 0)
    return jnp.where(upper, pltpu.roll(x, j, 0), pltpu.roll(x, 8 - j, 0))

def sort128(keys, pays, row, flip):
    bit=[(row & 1) != 0, (row & 2) != 0, (row & 4) != 0]
    def flipped(mask):
        for v in range(NV):
            keys[v] = jnp.where(mask, flip(keys[v]), keys[v])
    flipped(bit[0])
    for a,b in NET16:
        swap(keys,pays,a,b) if pays else swap_min(keys,a,b)
    for lvl in range(3):
        nxt = bit[lvl+1] if lvl < 2 else None
        flipped(jnp.logical_xor(bit[lvl], nxt) if nxt is not None else bit[lvl])
        for s in range(lvl,-1,-1):
            j=1<<s; up=bit[s]
            for v in range(NV):
                pk=partner(keys[v],j,up)
                if pays:
                    c=jnp.logical_xor(keys[v]>pk, up)
                    keys[v]=jnp.where(c,pk,keys[v])
                    for p in pays:
                        p[v]=jnp.where(c,partner(p[v],j,up),p[v])
                else:
                    keys[v]=jnp.where(up, jnp.maximum(keys[v],pk), jnp.minimum(keys[v],pk))
        for d in (8,4,2,1):
            for a in range(NV):
                if a & d == 0:
                    swap(keys,pays,a,a|d) if pays else swap_min(keys,a,a|d)

def before(parts, row):
    run=None; excl=[]
    for x in parts:
        excl.append(run)
        run = x if run is None else run + x
    x=run
    for j in (1,2,4):
        x = x + jnp.where(row >= j, pltpu.roll(x, j, 0), 0.0)
    ahead = jnp.where(row >= 1, pltpu.roll(x, 1, 0), 0.0)
    total = jnp.sum(run, axis=0, keepdims=True)
    return [ahead if e is None else ahead + e for e in excl], total

def collect_tile(r2t, mt):
    row = lax.broadcasted_iota(jnp.int32,(SUB,LAN),0)
    keys=[]; m=[]
    for v in range(NV):
        q = row*16+v
        x = r2t[v*8:(v+1)*8,:]
        keys.append((x*16384.0).astype(jnp.int32)*128+q)
        m.append(mt[v*8:(v+1)*8,:])
    sort128(keys,[m],row,lambda k: -1-k)
    q=[k & 127 for k in keys]
    r2=[(lax.shift_right_logical(k,7)).astype(jnp.float32)*(1.0/16384.0) + (0.5/16384.0) for k in keys]
    rad=[jnp.sqrt(x) for x in r2]
    r3=[a*b for a,b in zip(r2,rad)]
    r4=[a*a for a in r2]
    m1=[a*b for a,b in zip(m,rad)]
    m3=[a*b for a,b in zip(m,r3)]
    m4=[a*b for a,b in zip(m,r4)]
    m6=[a*b for a,b in zip(m3,r3)]
    m7=[a*b for a,b in zip(m3,r4)]
    p0,t0=before(m,row); p1,t1=before(m1,row)
    p3,t3=before(m3,row); p4,t4=before(m4,row)
    p6,_=before(m6,row); p7,_=before(m7,row)
    outs_r=[]; outs_m=[]; key2=[]
    for v in range(NV):
        gain = collect*((r4[v]*p3[v]-p7[v]) + 2.0*(r3[v]*p4[v]-rad[v]*p6[v]))
        loss = collect*(((t4-p4[v]) - r4[v]*(t0-p0[v])) + 2.0*(rad[v]*(t3-p3[v]) - r3[v]*(t1-p1[v])))
        x = r3[v] + time_step*gain
        y = jnp.exp(jnp.log(x)*(1.0/3.0))
        y = y - (y*y*y - x)/(3.0*y*y)
        outs_r.append(jnp.where(m[v]>0.0, y, 0.0))
        outs_m.append(m[v]*jnp.exp(-time_step*loss))
        key2.append((q[v]*128 + (row + v*8)).astype(jnp.float32))
    sort128(key2,[],row,lambda k: -k)
    rank=[(key2[v]-(row*16+v).astype(jnp.float32)*128.0) for v in range(NV)]
    cat=lambda l: jnp.concatenate(l,axis=0)
    return cat(outs_r),cat(outs_m),cat(rank)


W=3
UNROLL=8

def advect_kernel(tc,vc,uc,vw,wc,xlo_,xhi_,ylo_,yhi_,clo_,chi_,ot_,ov_,f,ax,ay,az,ad,s1,s2,ot,ov,xlo,xhi,ylo,yhi,clo,chi,sem,osem):
    nx,ny,_=tc.shape
    nt=ny//SUB+1
    small=[pltpu.make_async_copy(a,b,sem.at[5+i]) for i,(a,b) in enumerate(zip((xlo_,xhi_,ylo_,yhi_,clo_,chi_),(xlo,xhi,ylo,yhi,clo,chi)))]
    big=[pltpu.make_async_copy(c,f.at[i,pl.ds(W,nx),pl.ds(0,ny)],sem.at[i]) for i,c in enumerate((tc,vc,uc,vw,wc))]
    for c in small: c.start()
    for c in big[2:]+big[:2]: c.start()
    for c in small: c.wait()
    hi=slice(ny,ny+W); lo=slice(ny+SUB-W,ny+SUB)
    for i in range(5):
        f[i,0:W,0:ny,:]=xlo[i]
        f[i,W+nx:W+nx+W,0:ny,:]=xhi[i]
        for x in range(W):
            f[i,x,hi,:]=chi[0,i,x]; f[i,x,lo,:]=clo[0,i,x]
            f[i,W+nx+x,hi,:]=chi[1,i,x]; f[i,W+nx+x,lo,:]=clo[1,i,x]
    def sides(x,_):
        for i in range(5):
            f[i,W+x,hi,:]=yhi[i,pl.ds(x*W,W),:]
            f[i,W+x,lo,:]=ylo[i,pl.ds(x*W,W),:]
        return 0
    lax.fori_loop(0,nx,sides,0,unroll=4)
    for c in big[2:]: c.wait()
    scale=0.25*advect_step
    lane=lax.broadcasted_iota(jnp.int32,(SUB,LAN),1)
    first=lane==0; last=lane==LAN-1
    row=lax.broadcasted_iota(jnp.int32,(SUB,LAN),0)
    bottom=row==SUB-1; top=row==0
    rows=lambda t: pl.ds(t*SUB,SUB)
    near=pair_matrix()
    def ahead(tl):
        r=[pltpu.roll(x,SUB-1,0) for x in tl]
        return [jnp.where(bottom,r[(t+1)%nt],r[t]) for t in range(nt)]
    def behind(tl):
        r=[pltpu.roll(x,1,0) for x in tl]
        return [jnp.where(top,r[t-1],r[t]) for t in range(nt)]
    def pairs(tl):
        x=jnp.concatenate(tl,axis=0)
        hi=x.astype(jnp.bfloat16)
        lo=(x-hi.astype(jnp.float32)).astype(jnp.bfloat16)
        y=jnp.dot(jnp.concatenate([hi,lo],axis=1),near,preferred_element_type=jnp.float32)
        return [(y[k*SUB:(k+1)*SUB,:LAN],y[k*SUB:(k+1)*SUB,LAN:]) for k in range(len(tl))]
    def coef(g,_):
        x0=g*UNROLL
        zs=pairs([f[4,x0+p,rows(t),:] for p in range(UNROLL) for t in range(nt)])
        for p in range(UNROLL):
            x=x0+p
            xn=x+1
            for t in range(nt):
                ax[x,rows(t),:]=scale*(f[2,x,rows(t),:]+f[2,xn,rows(t),:])
            v=[f[3,x,rows(t),:] for t in range(nt)]
            for t,n in enumerate(ahead(v)):
                ay[x,rows(t),:]=scale*(v[t]+n)
            for t in range(nt):
                up,dn=zs[p*nt+t]
                az[x,rows(t),:]=jnp.where(last,0.0,scale*up)
                ad[x,rows(t),:]=jnp.where(first,0.0,scale*dn)
        return 0
    lax.fori_loop(0,pl.cdiv(nx+2*W,UNROLL),coef,0)
    def section(weight,src,dst,margin,count,after=lambda g: None):
        edge=tuple(ax[margin-1,rows(t),:]*(src[i,margin-1,rows(t),:]+src[i,margin,rows(t),:]) for i in range(2) for t in range(count))
        def planes(g,prev):
            x0=margin+g*UNROLL
            f0={(i,p):[src[i,x0+p,rows(t),:] for t in range(nt)] for i in range(2) for p in range(UNROLL+1)}
            zs=[pairs([f0[i,p][t] for p in range(UNROLL) for t in range(count)]) for i in range(2)]
            for p in range(UNROLL):
                x=x0+p; nxt=[]
                for i in range(2):
                    c=f0[i,p]; up=ahead(c)
                    gy=[ay[x,rows(t),:]*(c[t]+up[t]) for t in range(nt)]
                    dn=behind(gy)
                    for t in range(count):
                        gx=ax[x,rows(t),:]*(c[t]+f0[i,p+1][t])
                        zu,zd=zs[i][p*count+t]
                        d=(gx-prev[i*count+t])+(gy[t]-dn[t])+(az[x,rows(t),:]*zu-ad[x,rows(t),:]*zd)
                        dst(i,x,t,f[i,x,rows(t),:]-weight*d)
                        nxt.append(gx)
                prev=tuple(nxt)
            after(g)
            return prev
        lax.fori_loop(0,pl.cdiv(nx+2*W-2*margin,UNROLL),planes,edge)
    def put(buf):
        def g(i,x,t,val): buf[i,x,rows(t),:]=val
        return g
    def out(i,x,t,val):
        (ot,ov)[i][x-W,rows(t),:]=val
    for c in big[:2]: c.wait()
    section(1.0/3.0,f,put(s1),1,nt)
    section(0.5,s1,put(s2),2,nt)
    def drain(g):
        at=pl.ds(g*UNROLL,UNROLL)
        return [pltpu.make_async_copy(a.at[at],b.at[at],osem.at[i]) for i,(a,b) in enumerate(((ot,ot_),(ov,ov_)))]
    def flush(g):
        for c in drain(g): c.start()
    section(1.0,s2,out,3,nt-1,flush)
    for g in range(nx//UNROLL):
        for c in drain(g): c.wait()

def pair_matrix():
    k=lax.broadcasted_iota(jnp.int32,(2*LAN,2*LAN),0)
    n=lax.broadcasted_iota(jnp.int32,(2*LAN,2*LAN),1)
    z=jnp.where(k>=LAN,k-LAN,k)
    o=jnp.where(n>=LAN,n-LAN,n)
    other=jnp.where(n>=LAN,o-1,o+1)
    return jnp.where((z==o)|(z==other),1.0,0.0).astype(jnp.bfloat16)

def advect(t,v,u,w2,w3,*edges):
    nx,ny,nz=t.shape
    o=jax.ShapeDtypeStruct(t.shape,jnp.float32)
    ext=(pl.cdiv(nx+2*W,UNROLL)*UNROLL+SUB,ny+SUB,nz)
    ANY=pl.BlockSpec(memory_space=pl.ANY)
    return pl.pallas_call(advect_kernel,out_shape=(o,o),in_specs=[ANY]*11,out_specs=(ANY,ANY),
        scratch_shapes=[pltpu.VMEM((5,)+ext,jnp.float32)]+[pltpu.VMEM(ext,jnp.float32)]*4+[pltpu.VMEM((2,)+ext,jnp.float32)]*2
            +[pltpu.VMEM(t.shape,jnp.float32)]*2+[pltpu.VMEM(e.shape,jnp.float32) for e in edges]
            +[pltpu.SemaphoreType.DMA((11,)),pltpu.SemaphoreType.DMA((2,))],
        name="advect")(t,v,u,w2,w3,*edges)


def receive_kernel(src, mults, r2s, ro_ref, mo_ref, mrow, rrow):
    blocks = ro_ref.shape[0]

    def pull(b):
        s = src[b]
        mrow[pl.ds(b, 1), :] = mults[pl.ds(s, 1), :]
        rrow[pl.ds(b, 1), :] = r2s[pl.ds(s, 1), :]

    row_loop(blocks, 32, pull)

    def tile(t, _):
        sl = pl.ds(pl.multiple_of(t * LAN, LAN), LAN)
        r2 = jnp.transpose(rrow[sl, :])
        a, b, rank = collect_tile(r2, jnp.where(r2 > 0.0, jnp.transpose(mrow[sl, :]), 0.0))
        rank = jnp.transpose(rank).astype(jnp.int32)
        ro_ref[sl, :] = jnp.take_along_axis(jnp.transpose(a), rank, axis=1)
        mo_ref[sl, :] = jnp.take_along_axis(jnp.transpose(b), rank, axis=1)
        return 0

    lax.fori_loop(0, blocks // LAN, tile, 0)


def receive(src, mults, r2s):
    out = jax.ShapeDtypeStruct((BLK_DEV, LAN), jnp.float32)
    return pl.pallas_call(
        receive_kernel,
        out_shape=(out, out),
        in_specs=[SMEM(), VM(), VM()],
        out_specs=(VM(), VM()),
        scratch_shapes=[pltpu.VMEM((BLK_DEV, LAN), jnp.float32)] * 2,
        name="receive",
    )(src, mults, r2s)


def sources(mults):
    taken = mults[:, 0] > 0.0
    position = jnp.cumsum(taken.astype(jnp.int32)) - 1
    hit = (position[None, :] == jnp.arange(BLK_DEV, dtype=jnp.int32)[:, None]) & taken[None, :]
    return jnp.sum(jnp.where(hit, jnp.arange(mults.shape[0], dtype=jnp.int32)[None, :], 0), axis=1)


def exchange(rows, devices):
    moved = lax.all_to_all(
        rows.reshape((devices, -1) + rows.shape[1:]), ("gx", "gy"), 0, 0, tiled=True
    )
    return moved.reshape(rows.shape)


def shifts(axis):
    size = lax.axis_size(axis)
    up = [(i, (i + 1) % size) for i in range(size)]
    return up, [(j, i) for i, j in up]


def halos(xfirst, xlast, yfirst, ylast):
    ny = xfirst.shape[2]
    up, down = shifts("gx")
    xlo = lax.ppermute(xlast, "gx", up)
    xhi = lax.ppermute(xfirst, "gx", down)
    up, down = shifts("gy")
    ylo = lax.ppermute(ylast, "gy", up)
    yhi = lax.ppermute(yfirst, "gy", down)
    ends = jnp.stack([xlo, xhi])
    clo = lax.ppermute(ends[:, :, :, ny - W :], "gy", up)
    chi = lax.ppermute(ends[:, :, :, :W], "gy", down)
    return xlo, xhi, ylo, yhi, clo, chi


def body(
    tprime,
    vapor,
    wind_u,
    wind_v,
    wind_w,
    radius,
    min_radius,
    multiplicity,
    drop_counts,
    cell_index,
    move_list,
):
    devices = lax.axis_size("gx") * lax.axis_size("gy")
    levels = tprime.shape[2]
    slot = jnp.where(move_list >= 0, move_list, multiplicity.shape[0])
    column = lax.shift_right_logical(cell_index, levels.bit_length() - 1)
    level = cell_index & (levels - 1)
    mults = exchange(place(slot, multiplicity), devices)
    sent, ht, hv, ct, cv = home(
        slot, column, level, drop_counts, radius, min_radius, multiplicity, tprime, vapor
    )
    r2s = exchange(sent, devices)
    winds = (wind_u, wind_v, wind_w)
    heated_t, heated_v, *edges = scatter(
        column, level, cell_index, ht, hv, ct, cv, tprime, vapor, *winds
    )
    temperature_out, vapor_out = advect(heated_t, heated_v, *winds, *halos(*edges))
    radius_out, multiplicity_out = receive(sources(mults), mults, r2s)
    return (temperature_out, vapor_out, radius_out, multiplicity_out)


def solution(mesh):
    tile = P("gx", "gy", None)
    rows = P(("gx", "gy"), None)
    flat = P(("gx", "gy"))
    return jax.shard_map(
        body,
        mesh=mesh,
        in_specs=(tile,) * 5 + (rows,) * 3 + (flat,) * 3,
        out_specs=(tile, tile, rows, rows),
        check_vma=False,
    )
```

```python
import functools

import jax
import jax.numpy as jnp
from jax import lax
from jax.experimental import pallas as pl
from jax.experimental.pallas import tpu as pltpu
from jax.sharding import PartitionSpec as P

SUBSTEPS = 6
BLK_DEV = 512
LAN = 128
SUB = 8
NV = 16
collect = 1e-07
time_step = 2.0
advect_step = 0.6
clausius = 0.07; growth = 200.0 / 3.0; solute = 0.05; condense = 5e-07; latent = 10.0
SMEM=lambda: pl.BlockSpec(memory_space=pltpu.SMEM)
ANY=lambda: pl.BlockSpec(memory_space=pl.ANY)
VM=lambda: pl.BlockSpec(memory_space=pltpu.VMEM)

def row_loop(n, unroll, fn):
    def group(g,_):
        base=pl.multiple_of(g*unroll,unroll)
        for u in range(unroll):
            fn(base+u)
        return 0
    lax.fori_loop(0,n//unroll,group,0)

def staged(hbm, local, sem):
    copies = [pltpu.make_async_copy(x, y, sem.at[i]) for i, (x, y) in enumerate(zip(hbm, local))]
    for c in copies: c.start()
    return copies

def spare(n):
    rows = 1 << (n - 1).bit_length()
    return 2 * rows

def merge_kernel(cap,move_,r2_,mult_,send,move,r2s,mult,rows_r,rows_m,buf,sem):
    n=mult.shape[0]; wrap=spare(n)-1
    copies=staged((move_,r2_,mult_),(move,r2s,mult),sem)
    buf[:n,:]=jnp.zeros_like(mult); buf[n:2*n,:]=jnp.zeros_like(mult)
    for c in copies: c.wait()
    def tile(t,_):
        sl=pl.ds(pl.multiple_of(t*LAN,LAN),LAN)
        r2=jnp.transpose(r2s[sl,:])
        a,b,rank=collect_tile(r2,jnp.where(r2>0.0,jnp.transpose(mult[sl,:]),0.0))
        rank=jnp.transpose(rank).astype(jnp.int32)
        rows_r[sl,:]=jnp.take_along_axis(jnp.transpose(a),rank,axis=1)
        rows_m[sl,:]=jnp.take_along_axis(jnp.transpose(b),rank,axis=1)
        return 0
    lax.fori_loop(0,n//LAN,tile,0)
    def put(b):
        s=move[b]&wrap
        if cap&(cap-1):
            lead=lax.div(s,cap)
        else:
            lead=lax.shift_right_logical(s,cap.bit_length()-1)
        at=s+lead*cap
        buf[pl.ds(at,1),:]=rows_r[pl.ds(b,1),:]
        buf[pl.ds(at+cap,1),:]=rows_m[pl.ds(b,1),:]
    row_loop(n,32,put)
    last=pltpu.make_async_copy(buf.at[pl.ds(0,2*n)],send,sem.at[0])
    last.start(); last.wait()

def merge(cap,move,r2,mult):
    n=mult.shape[0]; F=lambda *d: pltpu.VMEM(d,jnp.float32)
    return pl.pallas_call(functools.partial(merge_kernel,cap),out_shape=jax.ShapeDtypeStruct((2*n,LAN),jnp.float32),
        in_specs=[ANY()]*3,out_specs=ANY(),
        scratch_shapes=[pltpu.SMEM((n,),jnp.int32)]+[F(n,LAN)]*4+[F(2*spare(n),LAN),pltpu.SemaphoreType.DMA((3,))],
        name="merge")(move,r2,mult)

def home_kernel(cell_,cells_,counts_,tp_,vp_,radius_,floor_,mult_,send,heat_,cell,cells,counts,tp,vp,radius,floor,mult,rows_t,rows_v,heat,sem):
    n=radius.shape[0]; g=n//LAN
    depth_bits=LAN.bit_length()-1
    copies=staged((cell_,tp_,vp_,cells_,counts_,radius_,floor_,mult_),(cell,tp,vp,cells,counts,radius,floor,mult),sem)
    for c in copies[:3]: c.wait()
    def fetch(b):
        c=lax.shift_right_logical(cell[b],depth_bits)
        rows_t[pl.ds(b,1),:]=tp[pl.ds(c,1),:]
        rows_v[pl.ds(b,1),:]=vp[pl.ds(c,1),:]
    row_loop(n,32,fetch)
    for c in copies[3:]: c.wait()
    depth=lax.broadcasted_iota(jnp.int32,(LAN,LAN),0)
    def tile(t,_):
        sl=pl.ds(pl.multiple_of(t*LAN,LAN),LAN)
        here=depth==(cells[pl.ds(t,1),:]&(LAN-1))
        temp0=jnp.sum(jnp.where(here,jnp.transpose(rows_t[sl,:]),0.0),axis=0,keepdims=True)
        wet0=jnp.sum(jnp.where(here,jnp.transpose(rows_v[sl,:]),0.0),axis=0,keepdims=True)
        r=jnp.transpose(radius[sl,:]); fl=jnp.transpose(floor[sl,:])
        alive=depth<counts[pl.ds(t,1),:]
        m=jnp.where(alive,jnp.transpose(mult[sl,:]),0.0)
        r2=r*r; f2=fl*fl; g3=(growth*solute)*(f2*fl)
        inv=lax.rsqrt(r2); mass=r2*(r2*inv)
        temp=temp0; wet=wet0
        for k in range(SUBSTEPS):
            sat=(1.0+wet)*jnp.exp(-clausius*temp)-1.0
            grown=jnp.maximum(r2+(growth*sat+g3*(inv*inv*inv)),f2)
            inv=lax.rsqrt(grown)
            new=grown*(grown*inv)
            condensed=jnp.sum(m*(new-mass),axis=0,keepdims=True)
            wet=wet-condense*condensed
            temp=temp+latent*condense*condensed
            r2=grown; mass=new
        heat[pl.ds(t,1),:]=temp-temp0; heat[pl.ds(g+t,1),:]=wet-wet0
        heat[pl.ds(2*g+t,1),:]=temp0; heat[pl.ds(3*g+t,1),:]=wet0
        rows_t[sl,:]=jnp.transpose(jnp.where(alive,r2,0.0))
        return 0
    lax.fori_loop(0,g,tile,0)
    first=pltpu.make_async_copy(heat,heat_,sem.at[1])
    first.start()
    last=pltpu.make_async_copy(rows_t,send,sem.at[0])
    last.start(); last.wait(); first.wait()

def home(cell,count,radius,floor,mult,tp,vp):
    n=radius.shape[0]; g=n//LAN
    cols=(tp.size//LAN,LAN); F=lambda *d: pltpu.VMEM(d,jnp.float32)
    return pl.pallas_call(home_kernel,
        out_shape=(jax.ShapeDtypeStruct(radius.shape,jnp.float32),jax.ShapeDtypeStruct((4*g,LAN),jnp.float32)),
        in_specs=[ANY()]*8,out_specs=(ANY(),)*2,
        scratch_shapes=[pltpu.SMEM((n,),jnp.int32)]+[pltpu.VMEM((g,LAN),jnp.int32)]*2+[F(*cols)]*2+[F(n,LAN)]*5
            +[F(4*g,LAN),pltpu.SemaphoreType.DMA((9,))],
        name="home")(cell,cell.reshape(g,LAN),count.reshape(g,LAN),tp.reshape(cols),vp.reshape(cols),radius,floor,mult)

def scatter_kernel(column,level,cells,heat,tp,vp,wu,wv,ww,ot,ov,xfirst,xlast,yfirst,ylast,vt,vv,acct,accv,spot,wlo,whi,sem):
    g=cells.shape[0]; n=g*LAN
    nx,ny=tp.shape[:2]
    winds=(wu,wv,ww)
    loads=[pltpu.make_async_copy(tp,ot,sem.at[0]),pltpu.make_async_copy(vp,ov,sem.at[1])]
    for i,w in enumerate(winds):
        loads+=[pltpu.make_async_copy(w.at[:,pl.ds(0,SUB)],wlo.at[i],sem.at[2+i]),
                pltpu.make_async_copy(w.at[:,pl.ds(ny-SUB,SUB)],whi.at[i],sem.at[5+i]),
                pltpu.make_async_copy(w.at[pl.ds(0,W)],xfirst.at[2+i],sem.at[8+i]),
                pltpu.make_async_copy(w.at[pl.ds(nx-W,W)],xlast.at[2+i],sem.at[11+i])]
    for c in loads: c.start()
    spread=lambda ref,t: jnp.transpose(jnp.broadcast_to(ref[pl.ds(t,1),:],(LAN,LAN)))
    spot[...]=cells[...].astype(jnp.float32)
    acct[...]=jnp.zeros_like(acct); accv[...]=jnp.zeros_like(accv)
    def source(t,_):
        c=spread(spot,t); a=spread(heat,t); b=spread(heat,g+t)
        for o in range(g):
            mine=spot[o:o+1,:]
            st=jnp.zeros((SUB,LAN),jnp.float32); sv=st
            for k in range(LAN//SUB):
                same=c[k*SUB:(k+1)*SUB,:]==mine
                st=st+jnp.where(same,a[k*SUB:(k+1)*SUB,:],0.0)
                sv=sv+jnp.where(same,b[k*SUB:(k+1)*SUB,:],0.0)
            acct[o*SUB:(o+1)*SUB,:]+=st
            accv[o*SUB:(o+1)*SUB,:]+=sv
        return 0
    lax.fori_loop(0,g,source,0)
    def rows(t,_):
        sl=pl.ds(pl.multiple_of(t*LAN,LAN),LAN)
        s8=pl.ds(pl.multiple_of(t*SUB,SUB),SUB)
        nt=heat[pl.ds(2*g+t,1),:]+jnp.sum(acct[s8,:],axis=0,keepdims=True)
        nv=heat[pl.ds(3*g+t,1),:]+jnp.sum(accv[s8,:],axis=0,keepdims=True)
        vt[sl,:]=jnp.transpose(jnp.broadcast_to(nt,(LAN,LAN)))
        vv[sl,:]=jnp.transpose(jnp.broadcast_to(nv,(LAN,LAN)))
        return 0
    lax.fori_loop(0,g,rows,0)
    for c in loads: c.wait()
    lane=lax.broadcasted_iota(jnp.int32,(1,LAN),1)
    flat_t=ot.reshape(nx*ny,LAN); flat_v=ov.reshape(nx*ny,LAN)
    def put(b):
        c=column[b]; hit=lane==level[b]
        pltpu.store(flat_t.at[pl.ds(c,1),:],vt[pl.ds(b,1),:],mask=hit)
        pltpu.store(flat_v.at[pl.ds(c,1),:],vv[pl.ds(b,1),:],mask=hit)
    row_loop(n,32,put)
    for i,o in enumerate((ot,ov)):
        xfirst[i]=o[0:W]; xlast[i]=o[nx-W:nx]
    def side(x,_):
        at=pl.ds(x*W,W)
        for i,o in enumerate((ot,ov)):
            yfirst[i,at,:]=o[x,0:W,:]; ylast[i,at,:]=o[x,ny-W:ny,:]
        for i in range(3):
            yfirst[2+i,at,:]=wlo[i,x,0:W,:]; ylast[2+i,at,:]=whi[i,x,SUB-W:SUB,:]
        return 0
    lax.fori_loop(0,nx,side,0,unroll=4)

def scatter(column,level,cell,heat,tp,vp,*winds):
    n=cell.shape[0]; g=n//LAN
    nx,ny,nz=tp.shape
    S=lambda *d: jax.ShapeDtypeStruct(d,jnp.float32)
    return pl.pallas_call(scatter_kernel,out_shape=(S(nx,ny,nz),)*2+(S(5,W,ny,nz),)*2+(S(5,nx*W,nz),)*2,
        in_specs=[SMEM()]*2+[VM()]*2+[ANY()]*5,out_specs=(VM(),)*6,
        scratch_shapes=[pltpu.VMEM((n,LAN),jnp.float32)]*2+[pltpu.VMEM((g*SUB,LAN),jnp.float32)]*2+[pltpu.VMEM((g,LAN),jnp.float32)]
            +[pltpu.VMEM((3,nx,SUB,nz),jnp.float32)]*2+[pltpu.SemaphoreType.DMA((14,))],
        name="scatter")(column,level,cell.reshape(g,LAN),heat,tp,vp,*winds)


def batcher(n):
    out=[]
    p=1
    while p<n:
        k=p
        while k>=1:
            for j in range(k%p, n-k, 2*k):
                for i in range(0, min(k, n-j-k)):
                    if (i+j)//(p*2)==(i+j+k)//(p*2):
                        out.append((i+j,i+j+k))
            k//=2
        p*=2
    return out
NET16=batcher(16)

def swap(keys, pays, a, b):
    c = keys[a] > keys[b]
    keys[a], keys[b] = jnp.where(c, keys[b], keys[a]), jnp.where(c, keys[a], keys[b])
    for p in pays:
        p[a], p[b] = jnp.where(c, p[b], p[a]), jnp.where(c, p[a], p[b])

def swap_min(keys, a, b):
    keys[a], keys[b] = jnp.minimum(keys[a], keys[b]), jnp.maximum(keys[a], keys[b])

def partner(x, j, upper):
    if j == 4:
        return pltpu.roll(x, 4, 0)
    return jnp.where(upper, pltpu.roll(x, j, 0), pltpu.roll(x, 8 - j, 0))

def sort128(keys, pays, row, flip):
    bit=[(row & 1) != 0, (row & 2) != 0, (row & 4) != 0]
    def flipped(mask):
        for v in range(NV):
            keys[v] = jnp.where(mask, flip(keys[v]), keys[v])
    flipped(bit[0])
    for a,b in NET16:
        swap(keys,pays,a,b) if pays else swap_min(keys,a,b)
    for lvl in range(3):
        nxt = bit[lvl+1] if lvl < 2 else None
        flipped(jnp.logical_xor(bit[lvl], nxt) if nxt is not None else bit[lvl])
        for s in range(lvl,-1,-1):
            j=1<<s; up=bit[s]
            for v in range(NV):
                pk=partner(keys[v],j,up)
                if pays:
                    c=jnp.logical_xor(keys[v]>pk, up)
                    keys[v]=jnp.where(c,pk,keys[v])
                    for p in pays:
                        p[v]=jnp.where(c,partner(p[v],j,up),p[v])
                else:
                    keys[v]=jnp.where(up, jnp.maximum(keys[v],pk), jnp.minimum(keys[v],pk))
        for d in (8,4,2,1):
            for a in range(NV):
                if a & d == 0:
                    swap(keys,pays,a,a|d) if pays else swap_min(keys,a,a|d)

def before(parts, row):
    run=None; excl=[]
    for x in parts:
        excl.append(run)
        run = x if run is None else run + x
    x=run
    for j in (1,2,4):
        x = x + jnp.where(row >= j, pltpu.roll(x, j, 0), 0.0)
    ahead = jnp.where(row >= 1, pltpu.roll(x, 1, 0), 0.0)
    total = jnp.sum(run, axis=0, keepdims=True)
    return [ahead if e is None else ahead + e for e in excl], total

def collect_tile(r2t, mt):
    row = lax.broadcasted_iota(jnp.int32,(SUB,LAN),0)
    keys=[]; m=[]
    for v in range(NV):
        q = row*16+v
        x = r2t[v*8:(v+1)*8,:]
        keys.append((x*16384.0).astype(jnp.int32)*128+q)
        m.append(mt[v*8:(v+1)*8,:])
    sort128(keys,[m],row,lambda k: -1-k)
    q=[k & 127 for k in keys]
    r2=[(lax.shift_right_logical(k,7)).astype(jnp.float32)*(1.0/16384.0) + (0.5/16384.0) for k in keys]
    rad=[jnp.sqrt(x) for x in r2]
    r3=[a*b for a,b in zip(r2,rad)]
    r4=[a*a for a in r2]
    m1=[a*b for a,b in zip(m,rad)]
    m3=[a*b for a,b in zip(m,r3)]
    m4=[a*b for a,b in zip(m,r4)]
    m6=[a*b for a,b in zip(m3,r3)]
    m7=[a*b for a,b in zip(m3,r4)]
    p0,t0=before(m,row); p1,t1=before(m1,row)
    p3,t3=before(m3,row); p4,t4=before(m4,row)
    p6,_=before(m6,row); p7,_=before(m7,row)
    outs_r=[]; outs_m=[]; key2=[]
    for v in range(NV):
        gain = collect*((r4[v]*p3[v]-p7[v]) + 2.0*(r3[v]*p4[v]-rad[v]*p6[v]))
        loss = collect*(((t4-p4[v]) - r4[v]*(t0-p0[v])) + 2.0*(rad[v]*(t3-p3[v]) - r3[v]*(t1-p1[v])))
        x = r3[v] + time_step*gain
        y = jnp.exp(jnp.log(x)*(1.0/3.0))
        y = y - (y*y*y - x)/(3.0*y*y)
        outs_r.append(jnp.where(m[v]>0.0, y, 0.0))
        outs_m.append(m[v]*jnp.exp(-time_step*loss))
        key2.append((q[v]*128 + (row + v*8)).astype(jnp.float32))
    sort128(key2,[],row,lambda k: -k)
    rank=[(key2[v]-(row*16+v).astype(jnp.float32)*128.0) for v in range(NV)]
    cat=lambda l: jnp.concatenate(l,axis=0)
    return cat(outs_r),cat(outs_m),cat(rank)


W=3
UNROLL=8

def advect_kernel(tc,vc,uc,vw,wc,xlo_,xhi_,ylo_,yhi_,clo_,chi_,ot_,ov_,f,ax,ay,az,ad,s1,s2,ot,ov,xlo,xhi,ylo,yhi,clo,chi,sem,osem):
    nx,ny,_=tc.shape
    nt=ny//SUB+1
    small=[pltpu.make_async_copy(a,b,sem.at[5+i]) for i,(a,b) in enumerate(zip((xlo_,xhi_,ylo_,yhi_,clo_,chi_),(xlo,xhi,ylo,yhi,clo,chi)))]
    big=[pltpu.make_async_copy(c,f.at[i,pl.ds(W,nx),pl.ds(0,ny)],sem.at[i]) for i,c in enumerate((tc,vc,uc,vw,wc))]
    for c in small: c.start()
    for c in big[2:]+big[:2]: c.start()
    for c in small: c.wait()
    hi=slice(ny,ny+W); lo=slice(ny+SUB-W,ny+SUB)
    for i in range(5):
        f[i,0:W,0:ny,:]=xlo[i]
        f[i,W+nx:W+nx+W,0:ny,:]=xhi[i]
        for x in range(W):
            f[i,x,hi,:]=chi[0,i,x]; f[i,x,lo,:]=clo[0,i,x]
            f[i,W+nx+x,hi,:]=chi[1,i,x]; f[i,W+nx+x,lo,:]=clo[1,i,x]
    def sides(x,_):
        for i in range(5):
            f[i,W+x,hi,:]=yhi[i,pl.ds(x*W,W),:]
            f[i,W+x,lo,:]=ylo[i,pl.ds(x*W,W),:]
        return 0
    lax.fori_loop(0,nx,sides,0,unroll=4)
    for c in big[2:]: c.wait()
    scale=0.25*advect_step
    lane=lax.broadcasted_iota(jnp.int32,(SUB,LAN),1)
    first=lane==0; last=lane==LAN-1
    row=lax.broadcasted_iota(jnp.int32,(SUB,LAN),0)
    bottom=row==SUB-1; top=row==0
    rows=lambda t: pl.ds(t*SUB,SUB)
    near=pair_matrix()
    def ahead(tl):
        r=[pltpu.roll(x,SUB-1,0) for x in tl]
        return [jnp.where(bottom,r[(t+1)%nt],r[t]) for t in range(nt)]
    def behind(tl):
        r=[pltpu.roll(x,1,0) for x in tl]
        return [jnp.where(top,r[t-1],r[t]) for t in range(nt)]
    def pairs(tl):
        x=jnp.concatenate(tl,axis=0)
        hi=x.astype(jnp.bfloat16)
        lo=(x-hi.astype(jnp.float32)).astype(jnp.bfloat16)
        y=jnp.dot(jnp.concatenate([hi,lo],axis=1),near,preferred_element_type=jnp.float32)
        return [(y[k*SUB:(k+1)*SUB,:LAN],y[k*SUB:(k+1)*SUB,LAN:]) for k in range(len(tl))]
    def coef(g,_):
        x0=g*UNROLL
        zs=pairs([f[4,x0+p,rows(t),:] for p in range(UNROLL) for t in range(nt)])
        for p in range(UNROLL):
            x=x0+p
            xn=x+1
            for t in range(nt):
                ax[x,rows(t),:]=scale*(f[2,x,rows(t),:]+f[2,xn,rows(t),:])
            v=[f[3,x,rows(t),:] for t in range(nt)]
            for t,n in enumerate(ahead(v)):
                ay[x,rows(t),:]=scale*(v[t]+n)
            for t in range(nt):
                up,dn=zs[p*nt+t]
                az[x,rows(t),:]=jnp.where(last,0.0,scale*up)
                ad[x,rows(t),:]=jnp.where(first,0.0,scale*dn)
        return 0
    lax.fori_loop(0,pl.cdiv(nx+2*W,UNROLL),coef,0)
    def section(weight,src,dst,margin,count,after=lambda g: None):
        edge=tuple(ax[margin-1,rows(t),:]*(src[i,margin-1,rows(t),:]+src[i,margin,rows(t),:]) for i in range(2) for t in range(count))
        def planes(g,prev):
            x0=margin+g*UNROLL
            f0={(i,p):[src[i,x0+p,rows(t),:] for t in range(nt)] for i in range(2) for p in range(UNROLL+1)}
            zs=[pairs([f0[i,p][t] for p in range(UNROLL) for t in range(count)]) for i in range(2)]
            for p in range(UNROLL):
                x=x0+p; nxt=[]
                for i in range(2):
                    c=f0[i,p]; up=ahead(c)
                    gy=[ay[x,rows(t),:]*(c[t]+up[t]) for t in range(nt)]
                    dn=behind(gy)
                    for t in range(count):
                        gx=ax[x,rows(t),:]*(c[t]+f0[i,p+1][t])
                        zu,zd=zs[i][p*count+t]
                        d=(gx-prev[i*count+t])+(gy[t]-dn[t])+(az[x,rows(t),:]*zu-ad[x,rows(t),:]*zd)
                        dst(i,x,t,f[i,x,rows(t),:]-weight*d)
                        nxt.append(gx)
                prev=tuple(nxt)
            after(g)
            return prev
        lax.fori_loop(0,pl.cdiv(nx+2*W-2*margin,UNROLL),planes,edge)
    def put(buf):
        def g(i,x,t,val): buf[i,x,rows(t),:]=val
        return g
    def out(i,x,t,val):
        (ot,ov)[i][x-W,rows(t),:]=val
    for c in big[:2]: c.wait()
    section(1.0/3.0,f,put(s1),1,nt)
    section(0.5,s1,put(s2),2,nt)
    def drain(g):
        at=pl.ds(g*UNROLL,UNROLL)
        return [pltpu.make_async_copy(a.at[at],b.at[at],osem.at[i]) for i,(a,b) in enumerate(((ot,ot_),(ov,ov_)))]
    def flush(g):
        for c in drain(g): c.start()
    section(1.0,s2,out,3,nt-1,flush)
    for g in range(nx//UNROLL):
        for c in drain(g): c.wait()

def pair_matrix():
    k=lax.broadcasted_iota(jnp.int32,(2*LAN,2*LAN),0)
    n=lax.broadcasted_iota(jnp.int32,(2*LAN,2*LAN),1)
    z=jnp.where(k>=LAN,k-LAN,k)
    o=jnp.where(n>=LAN,n-LAN,n)
    other=jnp.where(n>=LAN,o-1,o+1)
    return jnp.where((z==o)|(z==other),1.0,0.0).astype(jnp.bfloat16)

def advect(t,v,u,w2,w3,*edges):
    nx,ny,nz=t.shape
    o=jax.ShapeDtypeStruct(t.shape,jnp.float32)
    ext=(pl.cdiv(nx+2*W,UNROLL)*UNROLL+SUB,ny+SUB,nz)
    ANY=pl.BlockSpec(memory_space=pl.ANY)
    return pl.pallas_call(advect_kernel,out_shape=(o,o),in_specs=[ANY]*11,out_specs=(ANY,ANY),
        scratch_shapes=[pltpu.VMEM((5,)+ext,jnp.float32)]+[pltpu.VMEM(ext,jnp.float32)]*4+[pltpu.VMEM((2,)+ext,jnp.float32)]*2
            +[pltpu.VMEM(t.shape,jnp.float32)]*2+[pltpu.VMEM(e.shape,jnp.float32) for e in edges]
            +[pltpu.SemaphoreType.DMA((11,)),pltpu.SemaphoreType.DMA((2,))],
        name="advect")(t,v,u,w2,w3,*edges)


def receive_kernel(cap, src, rows, ro_ref, mo_ref):
    def pull(b):
        s = src[b]
        ro_ref[pl.ds(b, 1), :] = rows[pl.ds(s, 1), :]
        mo_ref[pl.ds(b, 1), :] = rows[pl.ds(s + cap, 1), :]

    row_loop(ro_ref.shape[0], 32, pull)


def receive(cap, src, rows):
    out = jax.ShapeDtypeStruct((BLK_DEV, LAN), jnp.float32)
    return pl.pallas_call(
        functools.partial(receive_kernel, cap),
        out_shape=(out, out),
        in_specs=[SMEM(), VM()],
        out_specs=(VM(), VM()),
        name="receive",
    )(src, rows)


def sources(rows, devices, cap):
    taken = rows.reshape(devices, 2, cap, LAN)[:, 0, :, 0].reshape(-1) > 0.0
    position = jnp.cumsum(taken.astype(jnp.int32)) - 1
    hit = (position[None, :] == jnp.arange(BLK_DEV, dtype=jnp.int32)[:, None]) & taken[None, :]
    slots = jnp.arange(devices * cap, dtype=jnp.int32)
    return jnp.sum(jnp.where(hit, (slots + slots // cap * cap)[None, :], 0), axis=1)


def exchange(rows, devices):
    moved = lax.all_to_all(
        rows.reshape((devices, -1) + rows.shape[1:]), ("gx", "gy"), 0, 0, tiled=True
    )
    return moved.reshape(rows.shape)


def shifts(axis):
    size = lax.axis_size(axis)
    up = [(i, (i + 1) % size) for i in range(size)]
    return up, [(j, i) for i, j in up]


def edge_halos(xfirst, xlast, yfirst, ylast):
    up, down = shifts("gx")
    xlo = lax.ppermute(xlast, "gx", up)
    xhi = lax.ppermute(xfirst, "gx", down)
    up, down = shifts("gy")
    return xlo, xhi, lax.ppermute(ylast, "gy", up), lax.ppermute(yfirst, "gy", down)


def corner_halos(xlo, xhi):
    ny = xlo.shape[2]
    up, down = shifts("gy")
    ends = jnp.stack([xlo, xhi])
    clo = lax.ppermute(ends[:, :, :, ny - W :], "gy", up)
    chi = lax.ppermute(ends[:, :, :, :W], "gy", down)
    return clo, chi


def body(
    tprime,
    vapor,
    wind_u,
    wind_v,
    wind_w,
    radius,
    min_radius,
    multiplicity,
    drop_counts,
    cell_index,
    move_list,
):
    devices = lax.axis_size("gx") * lax.axis_size("gy")
    levels = tprime.shape[2]
    column = lax.shift_right_logical(cell_index, levels.bit_length() - 1)
    level = cell_index & (levels - 1)
    winds = (wind_u, wind_v, wind_w)
    cap = (radius.shape[0] + devices - 1) // devices
    r2, heat = home(
        cell_index, drop_counts, radius, min_radius, multiplicity, tprime, vapor
    )
    heated_t, heated_v, *edges = scatter(column, level, cell_index, heat, tprime, vapor, *winds)
    edges, r2 = lax.optimization_barrier((edges, r2))
    xlo, xhi, ylo, yhi = edge_halos(*edges)
    xlo, xhi, ylo, yhi, sent = lax.optimization_barrier(
        (xlo, xhi, ylo, yhi, merge(cap, move_list, r2, multiplicity))
    )
    moved = exchange(sent, devices)
    clo, chi = corner_halos(xlo, xhi)
    temperature_out, vapor_out = advect(
        heated_t, heated_v, *winds, xlo, xhi, ylo, yhi, clo, chi
    )
    moved, temperature_out = lax.optimization_barrier((moved, temperature_out))
    radius_out, multiplicity_out = receive(cap, sources(moved, devices, cap), moved)
    return (temperature_out, vapor_out, radius_out, multiplicity_out)


def solution(mesh):
    tile = P("gx", "gy", None)
    rows = P(("gx", "gy"), None)
    flat = P(("gx", "gy"))
    return jax.shard_map(
        body,
        mesh=mesh,
        in_specs=(tile,) * 5 + (rows,) * 3 + (flat,) * 3,
        out_specs=(tile, tile, rows, rows),
        check_vma=False,
    )
```

```python
import functools

import jax
import jax.numpy as jnp
from jax import lax
from jax.experimental import pallas as pl
from jax.experimental.pallas import tpu as pltpu
from jax.sharding import PartitionSpec as P

SUBSTEPS = 6
BLK_DEV = 512
LAN = 128
SUB = 8
NV = 16
collect = 1e-07
time_step = 2.0
advect_step = 0.6
clausius = 0.07; growth = 200.0 / 3.0; solute = 0.05; condense = 5e-07; latent = 10.0
SMEM=lambda: pl.BlockSpec(memory_space=pltpu.SMEM)
ANY=lambda: pl.BlockSpec(memory_space=pl.ANY)
VM=lambda: pl.BlockSpec(memory_space=pltpu.VMEM)

def row_loop(n, unroll, fn):
    def group(g,_):
        base=pl.multiple_of(g*unroll,unroll)
        for u in range(unroll):
            fn(base+u)
        return 0
    lax.fori_loop(0,n//unroll,group,0)

def staged(hbm, local, sem):
    copies = [pltpu.make_async_copy(x, y, sem.at[i]) for i, (x, y) in enumerate(zip(hbm, local))]
    for c in copies: c.start()
    return copies

def spare(n):
    rows = 1 << (n - 1).bit_length()
    return 2 * rows

def merge_kernel(cap,move_,r2_,mult_,send,move,r2s,mult,rows_r,rows_m,buf,sem):
    n=mult.shape[0]; wrap=spare(n)-1
    copies=staged((move_,r2_,mult_),(move,r2s,mult),sem)
    buf[:n,:]=jnp.zeros_like(mult); buf[n:2*n,:]=jnp.zeros_like(mult)
    rows_r[:LAN,:]=jnp.zeros((LAN,LAN),jnp.float32); rows_m[:LAN,:]=jnp.zeros((LAN,LAN),jnp.float32)
    for c in copies: c.wait()
    def put(b):
        s=move[b]&wrap
        if cap&(cap-1):
            lead=lax.div(s,cap)
        else:
            lead=lax.shift_right_logical(s,cap.bit_length()-1)
        at=s+lead*cap
        buf[pl.ds(at,1),:]=rows_r[pl.ds(b,1),:]
        buf[pl.ds(at+cap,1),:]=rows_m[pl.ds(b,1),:]
    def tile(t,_):
        sl=pl.ds(pl.multiple_of(t*LAN,LAN),LAN)
        done=pl.multiple_of(jnp.maximum(t-1,0)*LAN,LAN)
        for u in range(LAN):
            put(done+u)
        r2=jnp.transpose(r2s[sl,:])
        a,b,rank=collect_tile(r2,jnp.where(r2>0.0,jnp.transpose(mult[sl,:]),0.0))
        rank=jnp.transpose(rank).astype(jnp.int32)
        rows_r[sl,:]=jnp.take_along_axis(jnp.transpose(a),rank,axis=1)
        rows_m[sl,:]=jnp.take_along_axis(jnp.transpose(b),rank,axis=1)
        return 0
    lax.fori_loop(0,n//LAN,tile,0)
    for u in range(LAN):
        put(n-LAN+u)
    last=pltpu.make_async_copy(buf.at[pl.ds(0,2*n)],send,sem.at[0])
    last.start(); last.wait()

def merge(cap,move,r2,mult):
    n=mult.shape[0]; F=lambda *d: pltpu.VMEM(d,jnp.float32)
    return pl.pallas_call(functools.partial(merge_kernel,cap),out_shape=jax.ShapeDtypeStruct((2*n,LAN),jnp.float32),
        in_specs=[ANY()]*3,out_specs=ANY(),
        scratch_shapes=[pltpu.SMEM((n,),jnp.int32)]+[F(n,LAN)]*4+[F(2*spare(n),LAN),pltpu.SemaphoreType.DMA((3,))],
        name="merge")(move,r2,mult)

def home_kernel(cell_,cells_,counts_,tp_,vp_,radius_,floor_,mult_,wu,wv,ww,send,ot_,ov_,xfirst,xlast,yfirst,ylast,cell,cells,counts,tp,vp,radius,floor,mult,rows_t,rows_v,heat,acct,accv,spot,wlo,whi,sem,wsem):
    n=radius.shape[0]; g=n//LAN
    depth_bits=LAN.bit_length()-1
    copies=staged((cell_,tp_,vp_,cells_,counts_,radius_,floor_,mult_),(cell,tp,vp,cells,counts,radius,floor,mult),sem)
    nx,ny=wu.shape[:2]
    loads=[]
    for i,w in enumerate((wu,wv,ww)):
        loads+=[pltpu.make_async_copy(w.at[:,pl.ds(0,SUB)],wlo.at[i],wsem.at[i]),
                pltpu.make_async_copy(w.at[:,pl.ds(ny-SUB,SUB)],whi.at[i],wsem.at[3+i]),
                pltpu.make_async_copy(w.at[pl.ds(0,W)],xfirst.at[2+i],wsem.at[6+i]),
                pltpu.make_async_copy(w.at[pl.ds(nx-W,W)],xlast.at[2+i],wsem.at[9+i])]
    for c in copies[:3]: c.wait()
    def fetch(b):
        c=lax.shift_right_logical(cell[b],depth_bits)
        rows_t[pl.ds(b,1),:]=tp[pl.ds(c,1),:]
        rows_v[pl.ds(b,1),:]=vp[pl.ds(c,1),:]
    row_loop(LAN,32,fetch)
    for c in copies[3:]: c.wait()
    for c in loads: c.start()
    depth=lax.broadcasted_iota(jnp.int32,(LAN,LAN),0)
    def tile(t,_):
        sl=pl.ds(pl.multiple_of(t*LAN,LAN),LAN)
        here=depth==(cells[pl.ds(t,1),:]&(LAN-1))
        near_t=rows_t[sl,:]; near_v=rows_v[sl,:]
        ahead=pl.multiple_of(jnp.minimum(t+1,g-1)*LAN,LAN)
        for u in range(LAN):
            fetch(ahead+u)
        temp0=jnp.sum(jnp.where(here,jnp.transpose(near_t),0.0),axis=0,keepdims=True)
        wet0=jnp.sum(jnp.where(here,jnp.transpose(near_v),0.0),axis=0,keepdims=True)
        r=jnp.transpose(radius[sl,:]); fl=jnp.transpose(floor[sl,:])
        alive=depth<counts[pl.ds(t,1),:]
        m=jnp.where(alive,jnp.transpose(mult[sl,:]),0.0)
        r2=r*r; f2=fl*fl; g3=(growth*solute)*(f2*fl)
        inv=lax.rsqrt(r2); mass=r2*(r2*inv)
        temp=temp0; wet=wet0
        for k in range(SUBSTEPS):
            sat=(1.0+wet)*jnp.exp(-clausius*temp)-1.0
            grown=jnp.maximum(r2+(growth*sat+g3*(inv*inv*inv)),f2)
            inv=lax.rsqrt(grown)
            new=grown*(grown*inv)
            condensed=jnp.sum(m*(new-mass),axis=0,keepdims=True)
            wet=wet-condense*condensed
            temp=temp+latent*condense*condensed
            r2=grown; mass=new
        heat[pl.ds(t,1),:]=temp-temp0; heat[pl.ds(g+t,1),:]=wet-wet0
        heat[pl.ds(2*g+t,1),:]=temp0; heat[pl.ds(3*g+t,1),:]=wet0
        radius[sl,:]=jnp.transpose(jnp.where(alive,r2,0.0))
        return 0
    lax.fori_loop(0,g,tile,0)
    last=pltpu.make_async_copy(radius,send,sem.at[0])
    last.start()
    spread=lambda ref,t: jnp.transpose(jnp.broadcast_to(ref[pl.ds(t,1),:],(LAN,LAN)))
    spot[...]=cells[...].astype(jnp.float32)
    acct[...]=jnp.zeros_like(acct); accv[...]=jnp.zeros_like(accv)
    def source(t,_):
        c=spread(spot,t); a=spread(heat,t); b=spread(heat,g+t)
        for o in range(g):
            mine=spot[o:o+1,:]
            st=jnp.zeros((SUB,LAN),jnp.float32); sv=st
            for k in range(LAN//SUB):
                same=c[k*SUB:(k+1)*SUB,:]==mine
                st=st+jnp.where(same,a[k*SUB:(k+1)*SUB,:],0.0)
                sv=sv+jnp.where(same,b[k*SUB:(k+1)*SUB,:],0.0)
            acct[o*SUB:(o+1)*SUB,:]+=st
            accv[o*SUB:(o+1)*SUB,:]+=sv
        return 0
    lax.fori_loop(0,g,source,0)
    def rows(t,_):
        sl=pl.ds(pl.multiple_of(t*LAN,LAN),LAN)
        s8=pl.ds(pl.multiple_of(t*SUB,SUB),SUB)
        nt=heat[pl.ds(2*g+t,1),:]+jnp.sum(acct[s8,:],axis=0,keepdims=True)
        nv=heat[pl.ds(3*g+t,1),:]+jnp.sum(accv[s8,:],axis=0,keepdims=True)
        rows_t[sl,:]=jnp.transpose(jnp.broadcast_to(nt,(LAN,LAN)))
        rows_v[sl,:]=jnp.transpose(jnp.broadcast_to(nv,(LAN,LAN)))
        return 0
    lax.fori_loop(0,g,rows,0)
    for c in loads: c.wait()
    lane=lax.broadcasted_iota(jnp.int32,(1,LAN),1)
    def put(b):
        x=cell[b]
        c=lax.shift_right_logical(x,LAN.bit_length()-1); hit=lane==(x&(LAN-1))
        pltpu.store(tp.at[pl.ds(c,1),:],rows_t[pl.ds(b,1),:],mask=hit)
        pltpu.store(vp.at[pl.ds(c,1),:],rows_v[pl.ds(b,1),:],mask=hit)
    row_loop(n,32,put)
    outs=staged((tp,vp),(ot_,ov_),wsem)
    ot=tp.reshape(nx,ny,LAN); ov=vp.reshape(nx,ny,LAN)
    for i,o in enumerate((ot,ov)):
        xfirst[i]=o[0:W]; xlast[i]=o[nx-W:nx]
    def side(x,_):
        at=pl.ds(x*W,W)
        for i,o in enumerate((ot,ov)):
            yfirst[i,at,:]=o[x,0:W,:]; ylast[i,at,:]=o[x,ny-W:ny,:]
        for i in range(3):
            yfirst[2+i,at,:]=wlo[i,x,0:W,:]; ylast[2+i,at,:]=whi[i,x,SUB-W:SUB,:]
        return 0
    lax.fori_loop(0,nx,side,0,unroll=4)
    last.wait()
    for c in outs: c.wait()

def home(cell,count,radius,floor,mult,tp,vp,*winds):
    n=radius.shape[0]; g=n//LAN
    nx,ny,nz=tp.shape
    cols=(nx*ny,nz); F=lambda *d: pltpu.VMEM(d,jnp.float32)
    S=lambda *d: jax.ShapeDtypeStruct(d,jnp.float32)
    r2,t,v,*edges=pl.pallas_call(home_kernel,
        out_shape=(S(n,LAN),S(*cols),S(*cols))+(S(5,W,ny,nz),)*2+(S(5,nx*W,nz),)*2,
        in_specs=[ANY()]*11,out_specs=(ANY(),)*3+(VM(),)*4,
        scratch_shapes=[pltpu.SMEM((n,),jnp.int32)]+[pltpu.VMEM((g,LAN),jnp.int32)]*2+[F(*cols)]*2+[F(n,LAN)]*5
            +[F(4*g,LAN)]+[F(g*SUB,LAN)]*2+[F(g,LAN)]+[F(3,nx,SUB,nz)]*2+[pltpu.SemaphoreType.DMA((8,)),pltpu.SemaphoreType.DMA((12,))],
        name="home")(cell,cell.reshape(g,LAN),count.reshape(g,LAN),tp.reshape(cols),vp.reshape(cols),radius,floor,mult,*winds)
    return r2,t.reshape(tp.shape),v.reshape(vp.shape),edges


def batcher(n):
    out=[]
    p=1
    while p<n:
        k=p
        while k>=1:
            for j in range(k%p, n-k, 2*k):
                for i in range(0, min(k, n-j-k)):
                    if (i+j)//(p*2)==(i+j+k)//(p*2):
                        out.append((i+j,i+j+k))
            k//=2
        p*=2
    return out
NET16=batcher(16)

def swap(keys, pays, a, b):
    c = keys[a] > keys[b]
    keys[a], keys[b] = jnp.where(c, keys[b], keys[a]), jnp.where(c, keys[a], keys[b])
    for p in pays:
        p[a], p[b] = jnp.where(c, p[b], p[a]), jnp.where(c, p[a], p[b])

def swap_min(keys, a, b):
    keys[a], keys[b] = jnp.minimum(keys[a], keys[b]), jnp.maximum(keys[a], keys[b])

def partner(x, j, upper):
    if j == 4:
        return pltpu.roll(x, 4, 0)
    return jnp.where(upper, pltpu.roll(x, j, 0), pltpu.roll(x, 8 - j, 0))

def sort128(keys, pays, row, flip):
    bit=[(row & 1) != 0, (row & 2) != 0, (row & 4) != 0]
    def flipped(mask):
        for v in range(NV):
            keys[v] = jnp.where(mask, flip(keys[v]), keys[v])
    flipped(bit[0])
    for a,b in NET16:
        swap(keys,pays,a,b) if pays else swap_min(keys,a,b)
    for lvl in range(3):
        nxt = bit[lvl+1] if lvl < 2 else None
        flipped(jnp.logical_xor(bit[lvl], nxt) if nxt is not None else bit[lvl])
        for s in range(lvl,-1,-1):
            j=1<<s; up=bit[s]
            for v in range(NV):
                pk=partner(keys[v],j,up)
                if pays:
                    c=jnp.logical_xor(keys[v]>pk, up)
                    keys[v]=jnp.where(c,pk,keys[v])
                    for p in pays:
                        p[v]=jnp.where(c,partner(p[v],j,up),p[v])
                else:
                    keys[v]=jnp.where(up, jnp.maximum(keys[v],pk), jnp.minimum(keys[v],pk))
        for d in (8,4,2,1):
            for a in range(NV):
                if a & d == 0:
                    swap(keys,pays,a,a|d) if pays else swap_min(keys,a,a|d)

def before(parts, row):
    run=None; excl=[]
    for x in parts:
        excl.append(run)
        run = x if run is None else run + x
    x=run
    for j in (1,2,4):
        x = x + jnp.where(row >= j, pltpu.roll(x, j, 0), 0.0)
    ahead = jnp.where(row >= 1, pltpu.roll(x, 1, 0), 0.0)
    total = jnp.sum(run, axis=0, keepdims=True)
    return [ahead if e is None else ahead + e for e in excl], total

def collect_tile(r2t, mt):
    row = lax.broadcasted_iota(jnp.int32,(SUB,LAN),0)
    keys=[]; m=[]
    for v in range(NV):
        q = row*16+v
        x = r2t[v*8:(v+1)*8,:]
        keys.append((x*16384.0).astype(jnp.int32)*128+q)
        m.append(mt[v*8:(v+1)*8,:])
    sort128(keys,[m],row,lambda k: -1-k)
    q=[k & 127 for k in keys]
    r2=[(lax.shift_right_logical(k,7)).astype(jnp.float32)*(1.0/16384.0) + (0.5/16384.0) for k in keys]
    rad=[jnp.sqrt(x) for x in r2]
    r3=[a*b for a,b in zip(r2,rad)]
    r4=[a*a for a in r2]
    m1=[a*b for a,b in zip(m,rad)]
    m3=[a*b for a,b in zip(m,r3)]
    m4=[a*b for a,b in zip(m,r4)]
    m6=[a*b for a,b in zip(m3,r3)]
    m7=[a*b for a,b in zip(m3,r4)]
    p0,t0=before(m,row); p1,t1=before(m1,row)
    p3,t3=before(m3,row); p4,t4=before(m4,row)
    p6,_=before(m6,row); p7,_=before(m7,row)
    outs_r=[]; outs_m=[]; key2=[]
    for v in range(NV):
        gain = collect*((r4[v]*p3[v]-p7[v]) + 2.0*(r3[v]*p4[v]-rad[v]*p6[v]))
        loss = collect*(((t4-p4[v]) - r4[v]*(t0-p0[v])) + 2.0*(rad[v]*(t3-p3[v]) - r3[v]*(t1-p1[v])))
        x = r3[v] + time_step*gain
        y = jnp.exp(jnp.log(x)*(1.0/3.0))
        y = y - (y*y*y - x)/(3.0*y*y)
        outs_r.append(jnp.where(m[v]>0.0, y, 0.0))
        outs_m.append(m[v]*jnp.exp(-time_step*loss))
        key2.append((q[v]*128 + (row + v*8)).astype(jnp.float32))
    sort128(key2,[],row,lambda k: -k)
    rank=[(key2[v]-(row*16+v).astype(jnp.float32)*128.0) for v in range(NV)]
    cat=lambda l: jnp.concatenate(l,axis=0)
    return cat(outs_r),cat(outs_m),cat(rank)


W=3
UNROLL=8

def advect_kernel(tc,vc,uc,vw,wc,xlo_,xhi_,ylo_,yhi_,clo_,chi_,ot_,ov_,f,ax,ay,az,ad,s1,s2,ot,ov,xlo,xhi,ylo,yhi,clo,chi,sem,osem):
    nx,ny,_=tc.shape
    nt=ny//SUB+1
    small=[pltpu.make_async_copy(a,b,sem.at[5+i]) for i,(a,b) in enumerate(zip((xlo_,xhi_,ylo_,yhi_,clo_,chi_),(xlo,xhi,ylo,yhi,clo,chi)))]
    big=[pltpu.make_async_copy(c,f.at[i,pl.ds(W,nx),pl.ds(0,ny)],sem.at[i]) for i,c in enumerate((tc,vc,uc,vw,wc))]
    for c in small: c.start()
    for c in big[2:]+big[:2]: c.start()
    for c in small: c.wait()
    hi=slice(ny,ny+W); lo=slice(ny+SUB-W,ny+SUB)
    for i in range(5):
        f[i,0:W,0:ny,:]=xlo[i]
        f[i,W+nx:W+nx+W,0:ny,:]=xhi[i]
        for x in range(W):
            f[i,x,hi,:]=chi[0,i,x]; f[i,x,lo,:]=clo[0,i,x]
            f[i,W+nx+x,hi,:]=chi[1,i,x]; f[i,W+nx+x,lo,:]=clo[1,i,x]
    def sides(x,_):
        for i in range(5):
            f[i,W+x,hi,:]=yhi[i,pl.ds(x*W,W),:]
            f[i,W+x,lo,:]=ylo[i,pl.ds(x*W,W),:]
        return 0
    lax.fori_loop(0,nx,sides,0,unroll=4)
    for c in big[2:]: c.wait()
    scale=0.25*advect_step
    lane=lax.broadcasted_iota(jnp.int32,(SUB,LAN),1)
    first=lane==0; last=lane==LAN-1
    row=lax.broadcasted_iota(jnp.int32,(SUB,LAN),0)
    bottom=row==SUB-1; top=row==0
    rows=lambda t: pl.ds(t*SUB,SUB)
    near=pair_matrix()
    def ahead(tl):
        r=[pltpu.roll(x,SUB-1,0) for x in tl]
        return [jnp.where(bottom,r[(t+1)%nt],r[t]) for t in range(nt)]
    def behind(tl):
        r=[pltpu.roll(x,1,0) for x in tl]
        return [jnp.where(top,r[t-1],r[t]) for t in range(nt)]
    def pairs(tl):
        x=jnp.concatenate(tl,axis=0)
        hi=x.astype(jnp.bfloat16)
        lo=(x-hi.astype(jnp.float32)).astype(jnp.bfloat16)
        y=jnp.dot(jnp.concatenate([hi,lo],axis=1),near,preferred_element_type=jnp.float32)
        return [(y[k*SUB:(k+1)*SUB,:LAN],y[k*SUB:(k+1)*SUB,LAN:]) for k in range(len(tl))]
    def coef(g,_):
        x0=g*UNROLL
        zs=pairs([f[4,x0+p,rows(t),:] for p in range(UNROLL) for t in range(nt)])
        for p in range(UNROLL):
            x=x0+p
            xn=x+1
            for t in range(nt):
                ax[x,rows(t),:]=scale*(f[2,x,rows(t),:]+f[2,xn,rows(t),:])
            v=[f[3,x,rows(t),:] for t in range(nt)]
            for t,n in enumerate(ahead(v)):
                ay[x,rows(t),:]=scale*(v[t]+n)
            for t in range(nt):
                up,dn=zs[p*nt+t]
                az[x,rows(t),:]=jnp.where(last,0.0,scale*up)
                ad[x,rows(t),:]=jnp.where(first,0.0,scale*dn)
        return 0
    lax.fori_loop(0,pl.cdiv(nx+2*W,UNROLL),coef,0)
    def section(weight,src,dst,margin,count,after=lambda g: None):
        edge=tuple(ax[margin-1,rows(t),:]*(src[i,margin-1,rows(t),:]+src[i,margin,rows(t),:]) for i in range(2) for t in range(count))
        def planes(g,prev):
            x0=margin+g*UNROLL
            f0={(i,p):[src[i,x0+p,rows(t),:] for t in range(nt)] for i in range(2) for p in range(UNROLL+1)}
            zs=[pairs([f0[i,p][t] for p in range(UNROLL) for t in range(count)]) for i in range(2)]
            for p in range(UNROLL):
                x=x0+p; nxt=[]
                for i in range(2):
                    c=f0[i,p]; up=ahead(c)
                    gy=[ay[x,rows(t),:]*(c[t]+up[t]) for t in range(nt)]
                    dn=behind(gy)
                    for t in range(count):
                        gx=ax[x,rows(t),:]*(c[t]+f0[i,p+1][t])
                        zu,zd=zs[i][p*count+t]
                        d=(gx-prev[i*count+t])+(gy[t]-dn[t])+(az[x,rows(t),:]*zu-ad[x,rows(t),:]*zd)
                        dst(i,x,t,f[i,x,rows(t),:]-weight*d)
                        nxt.append(gx)
                prev=tuple(nxt)
            after(g)
            return prev
        lax.fori_loop(0,pl.cdiv(nx+2*W-2*margin,UNROLL),planes,edge)
    def put(buf):
        def g(i,x,t,val): buf[i,x,rows(t),:]=val
        return g
    def out(i,x,t,val):
        (ot,ov)[i][x-W,rows(t),:]=val
    for c in big[:2]: c.wait()
    section(1.0/3.0,f,put(s1),1,nt)
    section(0.5,s1,put(s2),2,nt)
    def drain(g):
        at=pl.ds(g*UNROLL,UNROLL)
        return [pltpu.make_async_copy(a.at[at],b.at[at],osem.at[i]) for i,(a,b) in enumerate(((ot,ot_),(ov,ov_)))]
    def flush(g):
        for c in drain(g): c.start()
    section(1.0,s2,out,3,nt-1,flush)
    for g in range(nx//UNROLL):
        for c in drain(g): c.wait()

def pair_matrix():
    k=lax.broadcasted_iota(jnp.int32,(2*LAN,2*LAN),0)
    n=lax.broadcasted_iota(jnp.int32,(2*LAN,2*LAN),1)
    z=jnp.where(k>=LAN,k-LAN,k)
    o=jnp.where(n>=LAN,n-LAN,n)
    other=jnp.where(n>=LAN,o-1,o+1)
    return jnp.where((z==o)|(z==other),1.0,0.0).astype(jnp.bfloat16)

def advect(t,v,u,w2,w3,*edges):
    nx,ny,nz=t.shape
    o=jax.ShapeDtypeStruct(t.shape,jnp.float32)
    ext=(pl.cdiv(nx+2*W,UNROLL)*UNROLL+SUB,ny+SUB,nz)
    ANY=pl.BlockSpec(memory_space=pl.ANY)
    return pl.pallas_call(advect_kernel,out_shape=(o,o),in_specs=[ANY]*11,out_specs=(ANY,ANY),
        scratch_shapes=[pltpu.VMEM((5,)+ext,jnp.float32)]+[pltpu.VMEM(ext,jnp.float32)]*4+[pltpu.VMEM((2,)+ext,jnp.float32)]*2
            +[pltpu.VMEM(t.shape,jnp.float32)]*2+[pltpu.VMEM(e.shape,jnp.float32) for e in edges]
            +[pltpu.SemaphoreType.DMA((11,)),pltpu.SemaphoreType.DMA((2,))],
        name="advect")(t,v,u,w2,w3,*edges)


def receive_kernel(cap, place, rows, ro_ref, mo_ref, rbuf, mbuf):
    blocks = ro_ref.shape[0]
    slots = place.shape[0]

    def group(d, _):
        at = pl.multiple_of(d * cap, cap)
        for u in range(cap):
            to = place[at + u]
            rbuf[pl.ds(to, 1), :] = rows[pl.ds(2 * at + u, 1), :]
            mbuf[pl.ds(to, 1), :] = rows[pl.ds(2 * at + cap + u, 1), :]
        return 0

    lax.fori_loop(0, slots // cap, group, 0)
    ro_ref[...] = rbuf[:blocks, :]
    mo_ref[...] = mbuf[:blocks, :]


def receive(cap, place, rows):
    out = jax.ShapeDtypeStruct((BLK_DEV, LAN), jnp.float32)
    return pl.pallas_call(
        functools.partial(receive_kernel, cap),
        out_shape=(out, out),
        in_specs=[SMEM(), VM()],
        out_specs=(VM(), VM()),
        scratch_shapes=[pltpu.VMEM((BLK_DEV + SUB, LAN), jnp.float32)] * 2,
        name="receive",
    )(place, rows)


def places(rows, devices, cap):
    taken = rows.reshape(devices, 2, cap, LAN)[:, 0, :, 0].reshape(-1) > 0.0
    return jnp.where(taken, jnp.cumsum(taken.astype(jnp.int32)) - 1, BLK_DEV)


def exchange(rows, devices):
    moved = lax.all_to_all(
        rows.reshape((devices, -1) + rows.shape[1:]), ("gx", "gy"), 0, 0, tiled=True
    )
    return moved.reshape(rows.shape)


def shifts(axis):
    size = lax.axis_size(axis)
    up = [(i, (i + 1) % size) for i in range(size)]
    return up, [(j, i) for i, j in up]


def edge_halos(xfirst, xlast, yfirst, ylast):
    up, down = shifts("gx")
    xlo = lax.ppermute(xlast, "gx", up)
    xhi = lax.ppermute(xfirst, "gx", down)
    up, down = shifts("gy")
    return xlo, xhi, lax.ppermute(ylast, "gy", up), lax.ppermute(yfirst, "gy", down)


def corner_halos(xlo, xhi):
    ny = xlo.shape[2]
    up, down = shifts("gy")
    ends = jnp.stack([xlo, xhi])
    clo = lax.ppermute(ends[:, :, :, ny - W :], "gy", up)
    chi = lax.ppermute(ends[:, :, :, :W], "gy", down)
    return clo, chi


def body(
    tprime,
    vapor,
    wind_u,
    wind_v,
    wind_w,
    radius,
    min_radius,
    multiplicity,
    drop_counts,
    cell_index,
    move_list,
):
    devices = lax.axis_size("gx") * lax.axis_size("gy")
    winds = (wind_u, wind_v, wind_w)
    cap = (radius.shape[0] + devices - 1) // devices
    r2, heated_t, heated_v, edges = home(
        cell_index, drop_counts, radius, min_radius, multiplicity, tprime, vapor, *winds
    )
    edges, r2 = lax.optimization_barrier((edges, r2))
    xlo, xhi, ylo, yhi = edge_halos(*edges)
    xlo, xhi, ylo, yhi, sent = lax.optimization_barrier(
        (xlo, xhi, ylo, yhi, merge(cap, move_list, r2, multiplicity))
    )
    moved = exchange(sent, devices)
    clo, chi = corner_halos(xlo, xhi)
    temperature_out, vapor_out = advect(
        heated_t, heated_v, *winds, xlo, xhi, ylo, yhi, clo, chi
    )
    moved, temperature_out = lax.optimization_barrier((moved, temperature_out))
    radius_out, multiplicity_out = receive(cap, places(moved, devices, cap), moved)
    return (temperature_out, vapor_out, radius_out, multiplicity_out)


def solution(mesh):
    tile = P("gx", "gy", None)
    rows = P(("gx", "gy"), None)
    flat = P(("gx", "gy"))
    return jax.shard_map(
        body,
        mesh=mesh,
        in_specs=(tile,) * 5 + (rows,) * 3 + (flat,) * 3,
        out_specs=(tile, tile, rows, rows),
        check_vma=False,
    )
```

```python
import functools

import jax
import jax.numpy as jnp
from jax import lax
from jax.experimental import pallas as pl
from jax.experimental.pallas import tpu as pltpu
from jax.sharding import PartitionSpec as P

SUBSTEPS = 6
BLK_DEV = 512
LAN = 128
SUB = 8
NV = 16
collect = 1e-07
time_step = 2.0
advect_step = 0.6
clausius = 0.07; growth = 200.0 / 3.0; solute = 0.05; condense = 5e-07; latent = 10.0
SMEM=lambda: pl.BlockSpec(memory_space=pltpu.SMEM)
ANY=lambda: pl.BlockSpec(memory_space=pl.ANY)
VM=lambda: pl.BlockSpec(memory_space=pltpu.VMEM)

def row_loop(n, unroll, fn):
    def group(g,_):
        base=pl.multiple_of(g*unroll,unroll)
        for u in range(unroll):
            fn(base+u)
        return 0
    lax.fori_loop(0,n//unroll,group,0)

def staged(hbm, local, sem):
    copies = [pltpu.make_async_copy(x, y, sem.at[i]) for i, (x, y) in enumerate(zip(hbm, local))]
    for c in copies: c.start()
    return copies

def spare(n):
    rows = 1 << (n - 1).bit_length()
    return 2 * rows

def merge_kernel(cap,move_,r2_,mult_,send,move,r2s,mult,rows_r,rows_m,buf,sem):
    n=mult.shape[0]; wrap=spare(n)-1
    copies=staged((move_,r2_,mult_),(move,r2s,mult),sem)
    buf[:n,:]=jnp.zeros_like(mult); buf[n:2*n,:]=jnp.zeros_like(mult)
    rows_r[:LAN,:]=jnp.zeros((LAN,LAN),jnp.float32); rows_m[:LAN,:]=jnp.zeros((LAN,LAN),jnp.float32)
    for c in copies: c.wait()
    def put(b):
        s=move[b]&wrap
        if cap&(cap-1):
            lead=lax.div(s,cap)
        else:
            lead=lax.shift_right_logical(s,cap.bit_length()-1)
        at=s+lead*cap
        buf[pl.ds(at,1),:]=rows_r[pl.ds(b,1),:]
        buf[pl.ds(at+cap,1),:]=rows_m[pl.ds(b,1),:]
    def tile(t,_):
        sl=pl.ds(pl.multiple_of(t*LAN,LAN),LAN)
        done=pl.multiple_of(jnp.maximum(t-1,0)*LAN,LAN)
        for u in range(LAN):
            put(done+u)
        r2=jnp.transpose(r2s[sl,:])
        a,b,rank=collect_tile(r2,jnp.where(r2>0.0,jnp.transpose(mult[sl,:]),0.0))
        rank=jnp.transpose(rank).astype(jnp.int32)
        rows_r[sl,:]=jnp.take_along_axis(jnp.transpose(a),rank,axis=1)
        rows_m[sl,:]=jnp.take_along_axis(jnp.transpose(b),rank,axis=1)
        return 0
    lax.fori_loop(0,n//LAN,tile,0)
    for u in range(LAN):
        put(n-LAN+u)
    last=pltpu.make_async_copy(buf.at[pl.ds(0,2*n)],send,sem.at[0])
    last.start(); last.wait()

def merge(cap,move,r2,mult):
    n=mult.shape[0]; F=lambda *d: pltpu.VMEM(d,jnp.float32)
    return pl.pallas_call(functools.partial(merge_kernel,cap),out_shape=jax.ShapeDtypeStruct((2*n,LAN),jnp.float32),
        in_specs=[ANY()]*3,out_specs=ANY(),
        scratch_shapes=[pltpu.SMEM((n,),jnp.int32)]+[F(n,LAN)]*4+[F(2*spare(n),LAN),pltpu.SemaphoreType.DMA((3,))],
        name="merge")(move,r2,mult)

def home_kernel(cell_,cells_,counts_,tp_,vp_,radius_,floor_,mult_,wu,wv,ww,send,ot_,ov_,xfirst,xlast,yfirst,ylast,cell,cells,counts,tp,vp,radius,floor,mult,rows_t,rows_v,heat,acct,accv,spot,wlo,whi,sem,wsem):
    n=radius.shape[0]; g=n//LAN
    depth_bits=LAN.bit_length()-1
    copies=staged((cell_,tp_,vp_,cells_,counts_,radius_,floor_,mult_),(cell,tp,vp,cells,counts,radius,floor,mult),sem)
    nx,ny=wu.shape[:2]
    loads=[]
    for i,w in enumerate((wu,wv,ww)):
        loads+=[pltpu.make_async_copy(w.at[:,pl.ds(0,SUB)],wlo.at[i],wsem.at[i]),
                pltpu.make_async_copy(w.at[:,pl.ds(ny-SUB,SUB)],whi.at[i],wsem.at[3+i]),
                pltpu.make_async_copy(w.at[pl.ds(0,W)],xfirst.at[2+i],wsem.at[6+i]),
                pltpu.make_async_copy(w.at[pl.ds(nx-W,W)],xlast.at[2+i],wsem.at[9+i])]
    for c in copies[:3]: c.wait()
    def fetch(b):
        c=lax.shift_right_logical(cell[b],depth_bits)
        rows_t[pl.ds(b,1),:]=tp[pl.ds(c,1),:]
        rows_v[pl.ds(b,1),:]=vp[pl.ds(c,1),:]
    row_loop(LAN,32,fetch)
    for c in copies[3:]: c.wait()
    for c in loads: c.start()
    depth=lax.broadcasted_iota(jnp.int32,(LAN,LAN),0)
    def tile(t,_):
        sl=pl.ds(pl.multiple_of(t*LAN,LAN),LAN)
        here=depth==(cells[pl.ds(t,1),:]&(LAN-1))
        near_t=rows_t[sl,:]; near_v=rows_v[sl,:]
        ahead=pl.multiple_of(jnp.minimum(t+1,g-1)*LAN,LAN)
        for u in range(LAN):
            fetch(ahead+u)
        temp0=jnp.sum(jnp.where(here,jnp.transpose(near_t),0.0),axis=0,keepdims=True)
        wet0=jnp.sum(jnp.where(here,jnp.transpose(near_v),0.0),axis=0,keepdims=True)
        r=jnp.transpose(radius[sl,:]); fl=jnp.transpose(floor[sl,:])
        alive=depth<counts[pl.ds(t,1),:]
        m=jnp.where(alive,jnp.transpose(mult[sl,:]),0.0)
        r2=r*r; f2=fl*fl; g3=(growth*solute)*(f2*fl)
        inv=lax.rsqrt(r2); mass=r2*(r2*inv)
        temp=temp0; wet=wet0
        for k in range(SUBSTEPS):
            sat=(1.0+wet)*jnp.exp(-clausius*temp)-1.0
            grown=jnp.maximum(r2+(growth*sat+g3*(inv*inv*inv)),f2)
            inv=lax.rsqrt(grown)
            new=grown*(grown*inv)
            condensed=jnp.sum(m*(new-mass),axis=0,keepdims=True)
            wet=wet-condense*condensed
            temp=temp+latent*condense*condensed
            r2=grown; mass=new
        heat[pl.ds(t,1),:]=temp-temp0; heat[pl.ds(g+t,1),:]=wet-wet0
        heat[pl.ds(2*g+t,1),:]=temp0; heat[pl.ds(3*g+t,1),:]=wet0
        radius[sl,:]=jnp.transpose(jnp.where(alive,r2,0.0))
        return 0
    lax.fori_loop(0,g,tile,0)
    last=pltpu.make_async_copy(radius,send,sem.at[0])
    last.start()
    spread=lambda ref,t: jnp.transpose(jnp.broadcast_to(ref[pl.ds(t,1),:],(LAN,LAN)))
    spot[...]=cells[...].astype(jnp.float32)
    acct[...]=jnp.zeros_like(acct); accv[...]=jnp.zeros_like(accv)
    def source(t,_):
        c=spread(spot,t); a=spread(heat,t); b=spread(heat,g+t)
        for o in range(g):
            mine=spot[o:o+1,:]
            st=jnp.zeros((SUB,LAN),jnp.float32); sv=st
            for k in range(LAN//SUB):
                same=c[k*SUB:(k+1)*SUB,:]==mine
                st=st+jnp.where(same,a[k*SUB:(k+1)*SUB,:],0.0)
                sv=sv+jnp.where(same,b[k*SUB:(k+1)*SUB,:],0.0)
            acct[o*SUB:(o+1)*SUB,:]+=st
            accv[o*SUB:(o+1)*SUB,:]+=sv
        return 0
    lax.fori_loop(0,g,source,0)
    def rows(t,_):
        sl=pl.ds(pl.multiple_of(t*LAN,LAN),LAN)
        s8=pl.ds(pl.multiple_of(t*SUB,SUB),SUB)
        nt=heat[pl.ds(2*g+t,1),:]+jnp.sum(acct[s8,:],axis=0,keepdims=True)
        nv=heat[pl.ds(3*g+t,1),:]+jnp.sum(accv[s8,:],axis=0,keepdims=True)
        rows_t[sl,:]=jnp.transpose(jnp.broadcast_to(nt,(LAN,LAN)))
        rows_v[sl,:]=jnp.transpose(jnp.broadcast_to(nv,(LAN,LAN)))
        return 0
    lax.fori_loop(0,g,rows,0)
    for c in loads: c.wait()
    lane=lax.broadcasted_iota(jnp.int32,(1,LAN),1)
    def put(b):
        x=cell[b]
        c=lax.shift_right_logical(x,LAN.bit_length()-1); hit=lane==(x&(LAN-1))
        pltpu.store(tp.at[pl.ds(c,1),:],rows_t[pl.ds(b,1),:],mask=hit)
        pltpu.store(vp.at[pl.ds(c,1),:],rows_v[pl.ds(b,1),:],mask=hit)
    row_loop(n,32,put)
    outs=staged((tp,vp),(ot_,ov_),wsem)
    ot=tp.reshape(nx,ny,LAN); ov=vp.reshape(nx,ny,LAN)
    for i,o in enumerate((ot,ov)):
        xfirst[i]=o[0:W]; xlast[i]=o[nx-W:nx]
    def side(x,_):
        at=pl.ds(x*W,W)
        for i,o in enumerate((ot,ov)):
            yfirst[i,at,:]=o[x,0:W,:]; ylast[i,at,:]=o[x,ny-W:ny,:]
        for i in range(3):
            yfirst[2+i,at,:]=wlo[i,x,0:W,:]; ylast[2+i,at,:]=whi[i,x,SUB-W:SUB,:]
        return 0
    lax.fori_loop(0,nx,side,0,unroll=4)
    last.wait()
    for c in outs: c.wait()

def home(cell,count,radius,floor,mult,tp,vp,*winds):
    n=radius.shape[0]; g=n//LAN
    nx,ny,nz=tp.shape
    cols=(nx*ny,nz); F=lambda *d: pltpu.VMEM(d,jnp.float32)
    S=lambda *d: jax.ShapeDtypeStruct(d,jnp.float32)
    r2,t,v,*edges=pl.pallas_call(home_kernel,
        out_shape=(S(n,LAN),S(*cols),S(*cols))+(S(5,W,ny,nz),)*2+(S(5,nx*W,nz),)*2,
        in_specs=[ANY()]*11,out_specs=(ANY(),)*3+(VM(),)*4,
        scratch_shapes=[pltpu.SMEM((n,),jnp.int32)]+[pltpu.VMEM((g,LAN),jnp.int32)]*2+[F(*cols)]*2+[F(n,LAN)]*5
            +[F(4*g,LAN)]+[F(g*SUB,LAN)]*2+[F(g,LAN)]+[F(3,nx,SUB,nz)]*2+[pltpu.SemaphoreType.DMA((8,)),pltpu.SemaphoreType.DMA((12,))],
        name="home")(cell,cell.reshape(g,LAN),count.reshape(g,LAN),tp.reshape(cols),vp.reshape(cols),radius,floor,mult,*winds)
    return r2,t.reshape(tp.shape),v.reshape(vp.shape),edges


def batcher(n):
    out=[]
    p=1
    while p<n:
        k=p
        while k>=1:
            for j in range(k%p, n-k, 2*k):
                for i in range(0, min(k, n-j-k)):
                    if (i+j)//(p*2)==(i+j+k)//(p*2):
                        out.append((i+j,i+j+k))
            k//=2
        p*=2
    return out
NET16=batcher(16)

def swap(keys, pays, a, b):
    c = keys[a] > keys[b]
    keys[a], keys[b] = jnp.where(c, keys[b], keys[a]), jnp.where(c, keys[a], keys[b])
    for p in pays:
        p[a], p[b] = jnp.where(c, p[b], p[a]), jnp.where(c, p[a], p[b])

def swap_min(keys, a, b):
    keys[a], keys[b] = jnp.minimum(keys[a], keys[b]), jnp.maximum(keys[a], keys[b])

def partner(x, j, upper):
    if j == 4:
        return pltpu.roll(x, 4, 0)
    return jnp.where(upper, pltpu.roll(x, j, 0), pltpu.roll(x, 8 - j, 0))

def sort128(keys, pays, row, flip):
    bit=[(row & 1) != 0, (row & 2) != 0, (row & 4) != 0]
    def flipped(mask):
        for v in range(NV):
            keys[v] = jnp.where(mask, flip(keys[v]), keys[v])
    flipped(bit[0])
    for a,b in NET16:
        swap(keys,pays,a,b) if pays else swap_min(keys,a,b)
    for lvl in range(3):
        nxt = bit[lvl+1] if lvl < 2 else None
        flipped(jnp.logical_xor(bit[lvl], nxt) if nxt is not None else bit[lvl])
        for s in range(lvl,-1,-1):
            j=1<<s; up=bit[s]
            for v in range(NV):
                pk=partner(keys[v],j,up)
                if pays:
                    c=jnp.logical_xor(keys[v]>pk, up)
                    keys[v]=jnp.where(c,pk,keys[v])
                    for p in pays:
                        p[v]=jnp.where(c,partner(p[v],j,up),p[v])
                else:
                    keys[v]=jnp.where(up, jnp.maximum(keys[v],pk), jnp.minimum(keys[v],pk))
        for d in (8,4,2,1):
            for a in range(NV):
                if a & d == 0:
                    swap(keys,pays,a,a|d) if pays else swap_min(keys,a,a|d)

def before(parts, row):
    run=None; excl=[]
    for x in parts:
        excl.append(run)
        run = x if run is None else run + x
    x=run
    for j in (1,2,4):
        x = x + jnp.where(row >= j, pltpu.roll(x, j, 0), 0.0)
    ahead = jnp.where(row >= 1, pltpu.roll(x, 1, 0), 0.0)
    total = jnp.sum(run, axis=0, keepdims=True)
    return [ahead if e is None else ahead + e for e in excl], total

def collect_tile(r2t, mt):
    row = lax.broadcasted_iota(jnp.int32,(SUB,LAN),0)
    keys=[]; m=[]
    for v in range(NV):
        q = row*16+v
        x = r2t[v*8:(v+1)*8,:]
        keys.append((x*16384.0).astype(jnp.int32)*128+q)
        m.append(mt[v*8:(v+1)*8,:])
    sort128(keys,[m],row,lambda k: -1-k)
    q=[k & 127 for k in keys]
    r2=[(lax.shift_right_logical(k,7)).astype(jnp.float32)*(1.0/16384.0) + (0.5/16384.0) for k in keys]
    rad=[jnp.sqrt(x) for x in r2]
    r3=[a*b for a,b in zip(r2,rad)]
    r4=[a*a for a in r2]
    m1=[a*b for a,b in zip(m,rad)]
    m3=[a*b for a,b in zip(m,r3)]
    m4=[a*b for a,b in zip(m,r4)]
    m6=[a*b for a,b in zip(m3,r3)]
    m7=[a*b for a,b in zip(m3,r4)]
    p0,t0=before(m,row); p1,t1=before(m1,row)
    p3,t3=before(m3,row); p4,t4=before(m4,row)
    p6,_=before(m6,row); p7,_=before(m7,row)
    outs_r=[]; outs_m=[]; key2=[]
    for v in range(NV):
        gain = collect*((r4[v]*p3[v]-p7[v]) + 2.0*(r3[v]*p4[v]-rad[v]*p6[v]))
        loss = collect*(((t4-p4[v]) - r4[v]*(t0-p0[v])) + 2.0*(rad[v]*(t3-p3[v]) - r3[v]*(t1-p1[v])))
        x = r3[v] + time_step*gain
        y = jnp.exp(jnp.log(x)*(1.0/3.0))
        y = y - (y*y*y - x)/(3.0*y*y)
        outs_r.append(jnp.where(m[v]>0.0, y, 0.0))
        outs_m.append(m[v]*jnp.exp(-time_step*loss))
        key2.append((q[v]*128 + (row + v*8)).astype(jnp.float32))
    sort128(key2,[],row,lambda k: -k)
    rank=[(key2[v]-(row*16+v).astype(jnp.float32)*128.0) for v in range(NV)]
    cat=lambda l: jnp.concatenate(l,axis=0)
    return cat(outs_r),cat(outs_m),cat(rank)


W=3
UNROLL=8

def advect_kernel(tc,vc,uc,vw,wc,xlo_,xhi_,ylo_,yhi_,clo_,chi_,ot_,ov_,f,ax,ay,az,ad,s1,s2,ot,ov,xlo,xhi,ylo,yhi,clo,chi,sem,osem):
    nx,ny,_=tc.shape
    nt=ny//SUB+1
    small=[pltpu.make_async_copy(a,b,sem.at[5+i]) for i,(a,b) in enumerate(zip((xlo_,xhi_,ylo_,yhi_,clo_,chi_),(xlo,xhi,ylo,yhi,clo,chi)))]
    big=[pltpu.make_async_copy(c,f.at[i,pl.ds(W,nx),pl.ds(0,ny)],sem.at[i]) for i,c in enumerate((tc,vc,uc,vw,wc))]
    for c in small: c.start()
    for c in big[2:]+big[:2]: c.start()
    for c in small: c.wait()
    hi=slice(ny,ny+W); lo=slice(ny+SUB-W,ny+SUB)
    for i in range(5):
        f[i,0:W,0:ny,:]=xlo[i]
        f[i,W+nx:W+nx+W,0:ny,:]=xhi[i]
        for x in range(W):
            f[i,x,hi,:]=chi[0,i,x]; f[i,x,lo,:]=clo[0,i,x]
            f[i,W+nx+x,hi,:]=chi[1,i,x]; f[i,W+nx+x,lo,:]=clo[1,i,x]
    def sides(x,_):
        for i in range(5):
            f[i,W+x,hi,:]=yhi[i,pl.ds(x*W,W),:]
            f[i,W+x,lo,:]=ylo[i,pl.ds(x*W,W),:]
        return 0
    lax.fori_loop(0,nx,sides,0,unroll=4)
    for c in big[2:]: c.wait()
    scale=0.25*advect_step
    lane=lax.broadcasted_iota(jnp.int32,(SUB,LAN),1)
    first=lane==0; last=lane==LAN-1
    row=lax.broadcasted_iota(jnp.int32,(SUB,LAN),0)
    bottom=row==SUB-1; top=row==0
    rows=lambda t: pl.ds(t*SUB,SUB)
    near=pair_matrix()
    def ahead(tl):
        r=[pltpu.roll(x,SUB-1,0) for x in tl]
        return [jnp.where(bottom,r[(t+1)%nt],r[t]) for t in range(nt)]
    def behind(tl):
        r=[pltpu.roll(x,1,0) for x in tl]
        return [jnp.where(top,r[t-1],r[t]) for t in range(nt)]
    def pairs(tl):
        x=jnp.concatenate(tl,axis=0)
        hi=x.astype(jnp.bfloat16)
        lo=(x-hi.astype(jnp.float32)).astype(jnp.bfloat16)
        y=jnp.dot(jnp.concatenate([hi,lo],axis=1),near,preferred_element_type=jnp.float32)
        return [(y[k*SUB:(k+1)*SUB,:LAN],y[k*SUB:(k+1)*SUB,LAN:]) for k in range(len(tl))]
    def coef(g,_):
        x0=g*UNROLL
        zs=pairs([f[4,x0+p,rows(t),:] for p in range(UNROLL) for t in range(nt)])
        for p in range(UNROLL):
            x=x0+p
            xn=x+1
            for t in range(nt):
                ax[x,rows(t),:]=scale*(f[2,x,rows(t),:]+f[2,xn,rows(t),:])
            v=[f[3,x,rows(t),:] for t in range(nt)]
            for t,n in enumerate(ahead(v)):
                ay[x,rows(t),:]=scale*(v[t]+n)
            for t in range(nt):
                up,dn=zs[p*nt+t]
                az[x,rows(t),:]=jnp.where(last,0.0,scale*up)
                ad[x,rows(t),:]=jnp.where(first,0.0,scale*dn)
        return 0
    lax.fori_loop(0,pl.cdiv(nx+2*W,UNROLL),coef,0)
    def section(weight,src,dst,margin,count,after=lambda g: None):
        edge=tuple(ax[margin-1,rows(t),:]*(src[i,margin-1,rows(t),:]+src[i,margin,rows(t),:]) for i in range(2) for t in range(count))
        def planes(g,prev):
            x0=margin+g*UNROLL
            f0={(i,p):[src[i,x0+p,rows(t),:] for t in range(nt)] for i in range(2) for p in range(UNROLL+1)}
            zs=[pairs([f0[i,p][t] for p in range(UNROLL) for t in range(count)]) for i in range(2)]
            for p in range(UNROLL):
                x=x0+p; nxt=[]
                for i in range(2):
                    c=f0[i,p]; up=ahead(c)
                    gy=[ay[x,rows(t),:]*(c[t]+up[t]) for t in range(nt)]
                    dn=behind(gy)
                    for t in range(count):
                        gx=ax[x,rows(t),:]*(c[t]+f0[i,p+1][t])
                        zu,zd=zs[i][p*count+t]
                        d=(gx-prev[i*count+t])+(gy[t]-dn[t])+(az[x,rows(t),:]*zu-ad[x,rows(t),:]*zd)
                        dst(i,x,t,f[i,x,rows(t),:]-weight*d)
                        nxt.append(gx)
                prev=tuple(nxt)
            after(g)
            return prev
        lax.fori_loop(0,pl.cdiv(nx+2*W-2*margin,UNROLL),planes,edge)
    def put(buf):
        def g(i,x,t,val): buf[i,x,rows(t),:]=val
        return g
    def out(i,x,t,val):
        (ot,ov)[i][x-W,rows(t),:]=val
    for c in big[:2]: c.wait()
    section(1.0/3.0,f,put(s1),1,nt)
    section(0.5,s1,put(s2),2,nt)
    def drain(g):
        at=pl.ds(g*UNROLL,UNROLL)
        return [pltpu.make_async_copy(a.at[at],b.at[at],osem.at[i]) for i,(a,b) in enumerate(((ot,ot_),(ov,ov_)))]
    def flush(g):
        for c in drain(g): c.start()
    section(1.0,s2,out,3,nt-1,flush)
    for g in range(nx//UNROLL):
        for c in drain(g): c.wait()

def pair_matrix():
    k=lax.broadcasted_iota(jnp.int32,(2*LAN,2*LAN),0)
    n=lax.broadcasted_iota(jnp.int32,(2*LAN,2*LAN),1)
    z=jnp.where(k>=LAN,k-LAN,k)
    o=jnp.where(n>=LAN,n-LAN,n)
    other=jnp.where(n>=LAN,o-1,o+1)
    return jnp.where((z==o)|(z==other),1.0,0.0).astype(jnp.bfloat16)

def advect(t,v,u,w2,w3,*edges):
    nx,ny,nz=t.shape
    o=jax.ShapeDtypeStruct(t.shape,jnp.float32)
    ext=(pl.cdiv(nx+2*W,UNROLL)*UNROLL+SUB,ny+SUB,nz)
    ANY=pl.BlockSpec(memory_space=pl.ANY)
    return pl.pallas_call(advect_kernel,out_shape=(o,o),in_specs=[ANY]*11,out_specs=(ANY,ANY),
        scratch_shapes=[pltpu.VMEM((5,)+ext,jnp.float32)]+[pltpu.VMEM(ext,jnp.float32)]*4+[pltpu.VMEM((2,)+ext,jnp.float32)]*2
            +[pltpu.VMEM(t.shape,jnp.float32)]*2+[pltpu.VMEM(e.shape,jnp.float32) for e in edges]
            +[pltpu.SemaphoreType.DMA((11,)),pltpu.SemaphoreType.DMA((2,))],
        name="advect")(t,v,u,w2,w3,*edges)


def receive_kernel(cap, place_, rows_, ro_ref, mo_ref, place, rows, rbuf, mbuf, sem, psem):
    blocks = ro_ref.shape[0]
    groups = place.shape[0] // cap
    parts = 4 if groups % 4 == 0 else 1
    size = rows.shape[0] // parts
    first = pltpu.make_async_copy(place_, place, psem)
    first.start()
    loads = [
        pltpu.make_async_copy(
            rows_.at[pl.ds(i * size, size)], rows.at[pl.ds(i * size, size)], sem.at[i]
        )
        for i in range(parts)
    ]
    for c in loads:
        c.start()
    first.wait()

    def group(d, _):
        at = pl.multiple_of(d * cap, cap)
        for u in range(cap):
            to = place[at + u]
            rbuf[pl.ds(to, 1), :] = rows[pl.ds(2 * at + u, 1), :]
            mbuf[pl.ds(to, 1), :] = rows[pl.ds(2 * at + cap + u, 1), :]
        return 0

    for i, c in enumerate(loads):
        c.wait()
        lax.fori_loop(i * groups // parts, (i + 1) * groups // parts, group, 0)
    ro_ref[...] = rbuf[:blocks, :]
    mo_ref[...] = mbuf[:blocks, :]


def receive(cap, place, rows):
    out = jax.ShapeDtypeStruct((BLK_DEV, LAN), jnp.float32)
    return pl.pallas_call(
        functools.partial(receive_kernel, cap),
        out_shape=(out, out),
        in_specs=[ANY(), ANY()],
        out_specs=(VM(), VM()),
        scratch_shapes=[pltpu.SMEM(place.shape, jnp.int32), pltpu.VMEM(rows.shape, jnp.float32)]
        + [pltpu.VMEM((BLK_DEV + SUB, LAN), jnp.float32)] * 2
        + [pltpu.SemaphoreType.DMA((4,)), pltpu.SemaphoreType.DMA(())],
        name="receive",
    )(place, rows)


def places(rows, devices, cap):
    taken = rows.reshape(devices, 2, cap, LAN)[:, 0, :, 0].reshape(-1) > 0.0
    return jnp.where(taken, jnp.cumsum(taken.astype(jnp.int32)) - 1, BLK_DEV)


def exchange(rows, devices):
    moved = lax.all_to_all(
        rows.reshape((devices, -1) + rows.shape[1:]), ("gx", "gy"), 0, 0, tiled=True
    )
    return moved.reshape(rows.shape)


def shifts(axis):
    size = lax.axis_size(axis)
    up = [(i, (i + 1) % size) for i in range(size)]
    return up, [(j, i) for i, j in up]


def edge_halos(xfirst, xlast, yfirst, ylast):
    up, down = shifts("gx")
    xlo = lax.ppermute(xlast, "gx", up)
    xhi = lax.ppermute(xfirst, "gx", down)
    up, down = shifts("gy")
    return xlo, xhi, lax.ppermute(ylast, "gy", up), lax.ppermute(yfirst, "gy", down)


def corner_halos(xlo, xhi):
    ny = xlo.shape[2]
    up, down = shifts("gy")
    ends = jnp.stack([xlo, xhi])
    clo = lax.ppermute(ends[:, :, :, ny - W :], "gy", up)
    chi = lax.ppermute(ends[:, :, :, :W], "gy", down)
    return clo, chi


def body(
    tprime,
    vapor,
    wind_u,
    wind_v,
    wind_w,
    radius,
    min_radius,
    multiplicity,
    drop_counts,
    cell_index,
    move_list,
):
    devices = lax.axis_size("gx") * lax.axis_size("gy")
    winds = (wind_u, wind_v, wind_w)
    cap = (radius.shape[0] + devices - 1) // devices
    r2, heated_t, heated_v, edges = home(
        cell_index, drop_counts, radius, min_radius, multiplicity, tprime, vapor, *winds
    )
    edges, r2 = lax.optimization_barrier((edges, r2))
    xlo, xhi, ylo, yhi = edge_halos(*edges)
    xlo, xhi, ylo, yhi, sent = lax.optimization_barrier(
        (xlo, xhi, ylo, yhi, merge(cap, move_list, r2, multiplicity))
    )
    moved = exchange(sent, devices)
    clo, chi = corner_halos(xlo, xhi)
    temperature_out, vapor_out = advect(
        heated_t, heated_v, *winds, xlo, xhi, ylo, yhi, clo, chi
    )
    moved, temperature_out = lax.optimization_barrier((moved, temperature_out))
    radius_out, multiplicity_out = receive(cap, places(moved, devices, cap), moved)
    return (temperature_out, vapor_out, radius_out, multiplicity_out)


def solution(mesh):
    tile = P("gx", "gy", None)
    rows = P(("gx", "gy"), None)
    flat = P(("gx", "gy"))
    return jax.shard_map(
        body,
        mesh=mesh,
        in_specs=(tile,) * 5 + (rows,) * 3 + (flat,) * 3,
        out_specs=(tile, tile, rows, rows),
        check_vma=False,
    )
```
